128 devices in a mesh: rep: 1, dp: 128 (over x, y, z, core).
Axes of the slice: x: 4, y: 4, z: 4, core: 2. Of those that a mesh axis runs over, the one named last changes fastest.
Arguments:
- x: bfloat16 [128, 2048, 1024], P(('rep', 'dp'))
- dy: bfloat16 [128, 2048, 1024], P(('rep', 'dp'))
- w_gate: bfloat16 [2, 1024, 2816], P(None, 'dp')
- w_up: bfloat16 [2, 1024, 2816], P(None, 'dp')
- w_down: bfloat16 [2, 2816, 1024], P(None, 'dp')
Outputs:
- output 1: bfloat16 [128, 2048, 1024], P(('rep', 'dp'))
- output 2: bfloat16 [2, 1024, 2816], P('rep', 'dp')
- output 3: bfloat16 [2, 1024, 2816], P('rep', 'dp')
- output 4: bfloat16 [2, 2816, 1024], P('rep', 'dp')
All inputs are finite; a program needn't handle non-finite values.
Results may differ from the reference program's by a relative error of at most 0.018.
Values are sent between devices in bfloat16 or wider.
A program may use at most 1.5 GiB of HBM per device.

```python
import jax
import jax.numpy as jnp
from jax import lax

SEQUENCES = 128
TOKENS = 2048
D = 1024
FF = 2816
LAYERS = 2
NAMES = ("w_gate", "w_up", "w_down")
SHAPES = {"w_gate": (LAYERS, D, FF), "w_up": (LAYERS, D, FF), "w_down": (LAYERS, FF, D)}


def bump(key, n, height):
    away = (jnp.arange(n, dtype=jnp.int32) - jax.random.randint(key, (), 0, n, jnp.int32)) % n
    return jnp.where(away < n // 8, height, 1.0)


def together(key, own, strength):
    shared = jax.random.normal(key, own.shape[1:], jnp.float32)
    return (own + strength * shared) * lax.rsqrt(1 + strength * strength)


def setup_inputs(seed: int = 0, part: int = 0) -> dict:
    kx, kdy, ka, kb, kz, kf, kh, kl, *kw = jax.random.split(jax.random.key(seed), 8 + len(NAMES))
    kx, kdy, ka, kb = (jax.random.fold_in(k, part) for k in (kx, kdy, ka, kb))
    shape = (SEQUENCES, TOKENS, D)
    much_x, much_dy = jax.random.uniform(kz, (2,), jnp.float32, 0.0, 1.0)
    layers = 2.0 ** jax.random.uniform(kl, (LAYERS, 1, 1), jnp.float32, -1.0, 1.0)
    x = together(ka, jax.random.normal(kx, shape, jnp.float32), much_x) * bump(kf, D, 4.0)
    dy = together(kb, jax.random.normal(kdy, shape, jnp.float32), much_dy)
    drawn = {"x": x.astype(jnp.bfloat16), "dy": (dy * (SEQUENCES * TOKENS) ** -0.5).astype(jnp.bfloat16)}
    for key, name in zip(kw, NAMES, strict=True):
        w = jax.random.normal(key, SHAPES[name], jnp.float32) * SHAPES[name][1] ** -0.5
        drawn[name] = (w * {"w_gate": 1.0, "w_up": bump(kh, FF, 4.0), "w_down": layers}[name]).astype(jnp.bfloat16)
    return drawn


def matmul(a, w):
    return jnp.dot(a, w, preferred_element_type=jnp.float32).astype(jnp.bfloat16)


def normed(h):
    wide = h.astype(jnp.float32)
    scale = lax.rsqrt(jnp.mean(wide**2, -1, keepdims=True) + 1e-6)
    return (wide * scale).astype(jnp.bfloat16)


def layer(h, w):
    a = normed(h)
    gate = jnp.dot(a, w["w_gate"], preferred_element_type=jnp.float32)
    up = jnp.dot(a, w["w_up"], preferred_element_type=jnp.float32)
    return h + matmul((jax.nn.silu(gate) * up).astype(jnp.bfloat16), w["w_down"])


def stack(weights, h):
    return lax.scan(lambda h, w: (layer(h, w), None), h, weights)[0]


def reference(x, dy, w_gate, w_up, w_down):
    weights = dict(zip(NAMES, (w_gate, w_up, w_down), strict=True))

    def take(so_far, sequence):
        h, by_y = sequence
        _, back = jax.vjp(stack, weights, h)
        by_weights, by_h = back(by_y)
        return jax.tree.map(lambda total, term: total + term.astype(jnp.float32), so_far, by_weights), by_h

    none_yet = {name: jnp.zeros(w.shape, jnp.float32) for name, w in weights.items()}
    by_weights, by_x = lax.scan(take, none_yet, (x, dy))
    return (by_x, *(by_weights[name].astype(jnp.bfloat16) for name in NAMES))
```

```python
import functools

import jax
import jax.numpy as jnp
from jax import lax
from jax.experimental import pallas as pl
from jax.experimental.pallas import tpu as pltpu
from jax.sharding import PartitionSpec as P

bf=jnp.bfloat16
RING=4
COLS=256
LANES=128
ROWS=22
PAD=24
GROUP=8*ROWS
ALLOF=...
f32=jnp.float32
SUB=COLS
MESH=pl.DeviceIdType.MESH
W=8
ORDERS=((2,1,0),(0,2,1),(1,0,2))

def coords():
    me=lax.axis_index("dp")
    return (me//32, (me//8)%RING, (me//2)%RING), me%2

def dev(xyz,c):
    return {"dp": ((xyz[0]*RING+xyz[1])*RING+xyz[2])*2+c}

def moved(xyz,axis,to):
    return tuple(to if k==axis else v for k,v in enumerate(xyz))

def region(g,item,full,xyz,c,rows=slice(None),cols=slice(None)):
    ix=tuple(slice(None) if k in full else xyz[k] for k in range(3))
    return g.at[(item,*ix,c,rows,cols)]

def entry_barrier():
    xyz,c=coords()
    b=pltpu.get_barrier_semaphore()
    n=0
    for axis in range(3):
        for d in (1,2,3):
            pl.semaphore_signal(b,inc=1,device_id=dev(moved(xyz,axis,(xyz[axis]+d)%RING),c),device_id_type=MESH)
            n+=1
    pl.semaphore_signal(b,inc=1,device_id=dev(xyz,1-c),device_id_type=MESH)
    pl.semaphore_wait(b,n+1)

class Gather:
    STAGES=7
    def __init__(self,order,g,own,send,recv,local,halves):
        self.order,self.g,self.own,self.send,self.recv,self.local,self.halves=order,g,own,send,recv,local,halves
    def copies(self,stage,item):
        xyz,c=coords()
        a,b,last=self.order
        g=self.g
        slot=item%W
        sigma=1-2*c
        def copy(k,src,dst,to,tc=None):
            return pltpu.make_async_remote_copy(src_ref=src,dst_ref=dst,send_sem=self.send.at[slot,k],recv_sem=self.recv.at[slot,k],
                device_id=dev(to,c if tc is None else tc),device_id_type=MESH)
        if stage==0:
            mine=region(g,item,(),xyz,c)
            out=[copy(d-1,self.own(item),mine,moved(xyz,a,(xyz[a]+d)%RING)) for d in (1,2,3)]
            return out
        if stage in (1,3):
            axis,full=(b,(a,)) if stage==1 else (last,(a,b))
            r=region(g,item,full,xyz,c)
            k=3 if stage==1 else 7
            p,q=(xyz[axis]+sigma+RING)%RING,(xyz[axis]-sigma+RING)%RING
            return [copy(k,r,r,moved(xyz,axis,p)),copy(k+1,r,r,moved(xyz,axis,q))]
        if stage in (2,RING):
            axis,full=(b,(a,)) if stage==2 else (last,(a,b))
            k=5 if stage==2 else 9
            p,q=(xyz[axis]+sigma+RING)%RING,(xyz[axis]-sigma+RING)%RING
            (ra,ca),(rb,cb)=self.halves
            fromq=region(g,item,full,moved(xyz,axis,q),c,ra,ca)
            fromp=region(g,item,full,moved(xyz,axis,p),c,rb,cb)
            return [copy(k,fromq,fromq,moved(xyz,axis,p)),copy(k+1,fromp,fromp,moved(xyz,axis,q))]
        if stage==5:
            r=region(g,item,(0,1,2),xyz,c)
            return [copy(11,r,r,xyz,1-c)]
    def own_copy(self,item):
        xyz,c=coords()
        return pltpu.make_async_copy(self.own(item),region(self.g,item,(),xyz,c),self.local.at[item%W])
    def run(self,stage,item):
        if stage>0:
            for cp in self.copies(stage-1,item): cp.wait()
            if stage==1: self.own_copy(item).wait()
        if stage<6:
            for cp in self.copies(stage,item): cp.start()
            if stage==0: self.own_copy(item).start()

def ag_kernel(items,counts,wg,wu,wd,gg,gu,gd,wdp,*sems):
    L=wd.shape[0]
    wdp[ALLOF]=jnp.zeros_like(wdp)
    for l in range(L):
        wdp[l,0:ROWS,:]=wd[l]
    entry_barrier()
    ng,nd=counts
    half_c=((slice(None),pl.ds(0,LANES)),(slice(None),pl.ds(LANES,LANES)))
    half_r=((pl.ds(0,16),slice(None)),(pl.ds(16,8),slice(None)))
    own_g=lambda i: wg.at[i//ng,:,pl.ds(pl.multiple_of(i%ng*COLS,COLS),COLS)]
    own_u=lambda i: wu.at[i//ng,:,pl.ds(pl.multiple_of(i%ng*COLS,COLS),COLS)]
    own_d=lambda i: wdp.at[i//nd,:,pl.ds(pl.multiple_of(i%nd*LANES,LANES),LANES)]
    eg=Gather(ORDERS[0],gg,own_g,*sems[0:3],half_c)
    eu=Gather(ORDERS[1],gu,own_u,*sems[3:6],half_c)
    ed=Gather(ORDERS[2],gd,own_d,*sems[6:9],half_r)
    def tick(t,carry):
        for stage in reversed(range(7)):
            i=t-stage
            @pl.when((i>=0)&(i<items))
            def _():
                eg.run(stage,i); eu.run(stage,i)
                @pl.when(i%ng<nd)
                def _():
                    ed.run(stage,i//ng*nd+i%ng)
        return carry
    lax.fori_loop(0,items+6,tick,0)

def gather(wg,wu,wd):
    L,_,F=wg.shape; D=wd.shape[2]
    ng,nd=F//COLS,D//LANES
    assert nd<=ng or L==1
    items=L*ng
    sem=pltpu.SemaphoreType.DMA
    f=pl.pallas_call(functools.partial(ag_kernel,items,(ng,nd)),
        out_shape=[jax.ShapeDtypeStruct((L*ng,RING,RING,RING,2,8,COLS),bf)]*2+[jax.ShapeDtypeStruct((L*nd,RING,RING,RING,2,PAD,LANES),bf)],
        in_specs=[pl.BlockSpec(memory_space=pltpu.VMEM)]*3,
        out_specs=[pl.BlockSpec(memory_space=pl.ANY)]*3,
        scratch_shapes=[pltpu.VMEM((L,PAD,D),bf)]+[sem((W,12)),sem((W,12)),sem((W,))]*3,
        compiler_params=pltpu.CompilerParams(collective_id=0,has_side_effects=True),name="gather")
    return tuple(f(wg,wu,wd))

ALL=slice(None)
class Scatter:
    STAGES=7
    TW=RING
    @staticmethod
    def scratch(R,n,halves):
        (ra,ca),(rb,cb)=halves
        V=lambda *s: pltpu.VMEM(s,bf)
        return dict(ds=V(2,RING,RING,RING,R,n),dr=V(RING,RING,RING,RING,R,n),
            a1s=V(2,RING,RING,R,n),a1A=V(2,RING,RING,ra.size,ca.size),a1B=V(2,RING,RING,rb.size,cb.size),
            a2s=V(2,2,RING,RING,R,n),a2r=V(2,2,RING,RING,R,n),t1=pltpu.VMEM((2,RING,RING,R,n),f32),
            b1s=V(2,RING,R,n),b1A=V(2,RING,ra.size,ca.size),b1B=V(2,RING,rb.size,cb.size),
            b2s=V(2,2,RING,R,n),b2r=V(2,2,RING,R,n),t2=pltpu.VMEM((2,RING,R,n),f32),
            cs=V(2,3,R,n),cr=V(2,3,R,n),
            send=pltpu.SemaphoreType.DMA((2,12)),recv=pltpu.SemaphoreType.DMA((2,12)))
    def __init__(self,order,term,out,halves,refs):
        self.order,self.term,self.out,self.halves=order,term,out,halves
        self.__dict__.update(refs)
    def geometry(self):
        xyz,c=coords()
        cx,b,a=self.order
        sigma=1-2*c
        return xyz,c,a,b,cx,sigma
    def copies(self,stage,item):
        xyz,c,a,b,cx,sigma=self.geometry()
        s=item%2
        def copy(k,src,dst,to,tc=None):
            return pltpu.make_async_remote_copy(src_ref=src,dst_ref=dst,send_sem=self.send.at[s,k],recv_sem=self.recv.at[s,k],
                device_id=dev(to,c if tc is None else tc),device_id_type=MESH)
        if stage==0: return [copy(0,self.ds.at[s],self.dr.at[item%RING],xyz,1-c)]
        if stage in (1,3):
            axis=a if stage==1 else b
            k,src,A,B=(1,self.a1s,self.a1A,self.a1B) if stage==1 else (5,self.b1s,self.b1A,self.b1B)
            lead=(ALL,)*(2 if stage==1 else 1)
            p,q=(xyz[axis]+sigma+RING)%RING,(xyz[axis]-sigma+RING)%RING
            (ra,ca),(rb,cb)=self.halves
            return [copy(k,src.at[(s,*lead,ra,ca)],A.at[s],moved(xyz,axis,p)),copy(k+1,src.at[(s,*lead,rb,cb)],B.at[s],moved(xyz,axis,q))]
        if stage in (2,RING):
            axis=a if stage==2 else b
            k,src,dst=(3,self.a2s,self.a2r) if stage==2 else (7,self.b2s,self.b2r)
            p,q=(xyz[axis]+sigma+RING)%RING,(xyz[axis]-sigma+RING)%RING
            return [copy(k,src.at[s,0],dst.at[s,0],moved(xyz,axis,p)),copy(k+1,src.at[s,1],dst.at[s,1],moved(xyz,axis,q))]
        if stage==5:
            return [copy(8+d,self.cs.at[s,d-1],self.cr.at[s,d-1],moved(xyz,cx,(xyz[cx]+d)%RING)) for d in (1,2,3)]
    def run(self,stage,item):
        xyz,c,a,b,cx,sigma=self.geometry()
        s=item%2
        ts=item%self.TW; d4=item%RING
        (ra,ca),(rb,cb)=self.halves
        if stage>0:
            for cp in self.copies(stage-1,item): cp.wait()
        def plane(v):
            ix=tuple(v if k==a else ALL for k in range(3))
            return self.term[(ts,*ix,c)]+self.dr[(d4,*ix)].astype(f32)
        rem=[k for k in range(3) if k!=a]
        def line(v):
            ix=tuple(v if k==b else ALL for k in rem)
            return self.t1[(s,*ix)]
        if stage==0:
            self.ds[s]=self.term[ts,:,:,:,1-c].astype(bf)
        elif stage in (1,3):
            if stage==3:
                self.t1[s]=plane(xyz[a])+self.a2r[s,0].astype(f32)+self.a2r[s,1].astype(f32)
            axis,get,dst=(a,plane,self.a1s) if stage==1 else (b,line,self.b1s)
            dst[s]=get((xyz[axis]+2)%RING).astype(bf)
        elif stage in (2,RING):
            axis,get,dst,A,B,nd=(a,plane,self.a2s,self.a1A,self.a1B,2) if stage==2 else (b,line,self.b2s,self.b1A,self.b1B,1)
            lead=(ALL,)*nd
            p,q=(xyz[axis]+sigma+RING)%RING,(xyz[axis]-sigma+RING)%RING
            vp,vq=get(p),get(q)
            st=lambda k,r,cl,v: dst.__setitem__((s,k,*lead,r,cl),v.astype(bf))
            cut=lambda v,r,cl: v[(*lead,slice(r.start,r.start+r.size),slice(cl.start,cl.start+cl.size))]
            st(0,ra,ca,cut(vp,ra,ca)+A[s].astype(f32)); st(0,rb,cb,cut(vp,rb,cb))
            st(1,ra,ca,cut(vq,ra,ca)); st(1,rb,cb,cut(vq,rb,cb)+B[s].astype(f32))
        elif stage==5:
            self.t2[s]=line(xyz[b])+self.b2r[s,0].astype(f32)+self.b2r[s,1].astype(f32)
            for d in (1,2,3):
                self.cs[s,d-1]=self.t2[s,(xyz[cx]+d)%RING].astype(bf)
        else:
            v=self.t2[s,xyz[cx]]
            for d in range(3): v=v+self.cr[s,d].astype(f32)
            self.out(item,v.astype(bf))
        if stage<6:
            for cp in self.copies(stage,item): cp.start()

HC=((pl.ds(0,8),pl.ds(0,LANES)),(pl.ds(0,8),pl.ds(LANES,LANES)))
HR=((pl.ds(0,16),pl.ds(0,LANES)),(pl.ds(16,8),pl.ds(0,LANES)))

def rs_kernel(L,ng,nd,tg0,tg1,tu0,tu1,td0,td1,og,ou,od,odp,vg,vu,vd,lsem,*scr):
    n1=len(Scatter.scratch(8,COLS,HC))
    keys=list(Scatter.scratch(8,COLS,HC))
    pack=lambda k: dict(zip(keys,scr[k*n1:(k+1)*n1],strict=True))
    entry_barrier()
    items=L*ng
    lay=lambda i: L-1-i//ng
    idx=lambda i: lay(i)*ng+i%ng
    cols=lambda i: pl.ds(pl.multiple_of(i%ng*COLS,COLS),COLS)
    def outg(i,v): og[lay(i),:,cols(i)]=v
    def outu(i,v): ou[lay(i),:,cols(i)]=v
    def outd(k,v): odp[L-1-k//nd,:,pl.ds(pl.multiple_of(k%nd*LANES,LANES),LANES)]=v
    eg=Scatter(ORDERS[0],vg,outg,HC,pack(0))
    eu=Scatter(ORDERS[1],vu,outu,HC,pack(1))
    ed=Scatter(ORDERS[2],vd,outd,HR,pack(2))
    dk=lambda i: i//ng*nd+i%ng
    didx=lambda k: (L-1-k//nd)*nd+k%nd
    def load(m,i,go):
        v=(vg,vu,vd)[m]
        k,slot=(i%ng,i%RING) if m<2 else (i%ng,dk(i)%RING)
        for l,src in enumerate(((tg0,tg1),(tu0,tu1),(td0,td1))[m]):
            @pl.when(lay(i)==l)
            def _():
                cp=pltpu.make_async_copy(src.at[k],v.at[slot],lsem.at[m,i%2])
                cp.start() if go else cp.wait()
    def loads(i,go):
        load(0,i,go); load(1,i,go)
        @pl.when(i%ng<nd)
        def _(): load(2,i,go)
    loads(0,True)
    def tick(t,carry):
        for stage in reversed(range(7)):
            i=t-stage
            @pl.when((i>=0)&(i<items))
            def _():
                if stage==0: loads(i,False)
                eg.run(stage,i); eu.run(stage,i)
                @pl.when(i%ng<nd)
                def _(): ed.run(stage,dk(i))
        @pl.when(t+1<items)
        def _(): loads(t+1,True)
        return carry
    lax.fori_loop(0,items+6,tick,0)
    od[ALLOF]=odp[:,0:ROWS,:]

def reduce_scatter(tg,tu,td,L,F,D):
    ng,nd=F//COLS,D//LANES
    def flat(R,n,h): return list(Scatter.scratch(R,n,h).values())
    f=pl.pallas_call(functools.partial(rs_kernel,L,ng,nd),
        out_shape=[jax.ShapeDtypeStruct((L,8,F),bf)]*2+[jax.ShapeDtypeStruct((L,ROWS,D),bf)],
        in_specs=[pl.BlockSpec(memory_space=pl.ANY)]*6,
        out_specs=[pl.BlockSpec(memory_space=pltpu.VMEM)]*3,
        scratch_shapes=[pltpu.VMEM((L,PAD,D),bf),pltpu.VMEM((RING,RING,RING,RING,2,8,COLS),f32),pltpu.VMEM((RING,RING,RING,RING,2,8,COLS),f32),pltpu.VMEM((RING,RING,RING,RING,2,PAD,LANES),f32),
            pltpu.SemaphoreType.DMA((3,2))]+flat(8,COLS,HC)*2+flat(PAD,LANES,HR),
        compiler_params=pltpu.CompilerParams(collective_id=1,has_side_effects=True,vmem_limit_bytes=60<<20),name="scatter")
    return tuple(f(*tg,*tu,*td))

M,D,F=2048,1024,2816
NG=11
BM=COLS
def dot(a,b,ca=1,cb=0):
    return lax.dot_general(a,b,(((ca,),(cb,)),((),())),preferred_element_type=f32)
CP=lambda mb: pltpu.CompilerParams(vmem_limit_bytes=mb<<20)
S=jax.ShapeDtypeStruct
def normed(h):
    wide=h.astype(f32)
    return (wide*lax.rsqrt(jnp.mean(wide*wide,-1,keepdims=True)+1e-6)).astype(bf)
def cost(n): return pl.CostEstimate(flops=2*M*D*F*n,bytes_accessed=1<<PAD,transcendentals=0)

def norm_kernel(h_ref,a_ref,at_ref):
    a=normed(h_ref[ALLOF])
    a_ref[ALLOF]=a
    at_ref[ALLOF]=a.T
def norm(h):
    return pl.pallas_call(norm_kernel,grid=(M//BM,),in_specs=[pl.BlockSpec((BM,D),lambda i:(i,0))],
        out_specs=[pl.BlockSpec((BM,D),lambda i:(i,0)),pl.BlockSpec((D,BM),lambda i:(0,i))],
        out_shape=[S((M,D),bf),S((D,M),bf)],compiler_params=CP(32),name="norm")(h)

def gu_kernel(a_ref,wg_ref,wu_ref,g_ref,u_ref,pt_ref):
    for r in range(0,M,SUB):
        rows=pl.ds(r,SUB)
        g=dot(a_ref[rows,:],wg_ref[0])
        u=dot(a_ref[rows,:],wu_ref[0])
        s=jax.nn.sigmoid(g)
        b=g*s
        g_ref[0,rows,:]=u*(s+b*(1-s)); u_ref[0,rows,:]=b
        pt_ref[:,rows]=(b*u).astype(bf).T
def gate_up(l,a,wg,wu):
    return pl.pallas_call(gu_kernel,grid=(NG,),in_specs=[pl.BlockSpec((M,D),lambda j:(0,0)),pl.BlockSpec((1,D,COLS),lambda j:(l*NG+j,0,0)),pl.BlockSpec((1,D,COLS),lambda j:(l*NG+j,0,0))],
        out_specs=[pl.BlockSpec((1,M,COLS),lambda j:(j,0,0))]*2+[pl.BlockSpec((COLS,M),lambda j:(j,0))],
        out_shape=[S((NG,M,COLS),f32)]*2+[S((F,M),bf)],compiler_params=CP(60),cost_estimate=cost(2),name="gate_up")(a,wg,wu)

def compact_kernel(w_ref,o_ref):
    def group(k,c):
        v=w_ref[0,pl.ds(k*8,8)].astype(f32)
        o_ref[pl.ds(pl.multiple_of(k*GROUP,GROUP),GROUP),:]=jnp.concatenate([v[d,0:ROWS] for d in range(8)],0).astype(bf)
        return c
    lax.fori_loop(0,16,group,0)
def compact(w):
    n=w.shape[0]//2
    return [pl.pallas_call(compact_kernel,grid=(n,),in_specs=[pl.BlockSpec((1,LANES,PAD,LANES),lambda k:(l*n+k,0,0,0))],
        out_specs=pl.BlockSpec((F,LANES),lambda k:(0,k)),out_shape=S((F,D),bf),compiler_params=CP(32),name="compact")(w) for l in range(2)]

def down_kernel(pt_ref,w_ref,h_ref,h1_ref,a_ref,at_ref):
    y=dot(pt_ref[ALLOF],w_ref[ALLOF],0,0).astype(bf)
    h=h_ref[ALLOF]+y
    h1_ref[ALLOF]=h
    a=normed(h)
    a_ref[ALLOF]=a
    at_ref[ALLOF]=a.T
def down(pt,w,h):
    return pl.pallas_call(down_kernel,grid=(M//BM,),in_specs=[pl.BlockSpec((F,BM),lambda i:(0,i)),pl.BlockSpec((F,D),lambda i:(0,0)),pl.BlockSpec((BM,D),lambda i:(i,0))],
        out_specs=[pl.BlockSpec((BM,D),lambda i:(i,0))]*2+[pl.BlockSpec((D,BM),lambda i:(0,i))],
        out_shape=[S((M,D),bf)]*2+[S((D,M),bf)],compiler_params=CP(60),cost_estimate=cost(1),name="down")(pt,w,h)

def wd_kernel(pt_ref,dh_ref,t_ref,acc):
    acc[ALLOF]=dot(pt_ref[ALLOF],dh_ref[ALLOF])
    def group(k,c):
        for half in range(2):
            v=acc[pl.ds(pl.multiple_of(k*GROUP,GROUP),GROUP),pl.ds(half*LANES,LANES)]
            for d in range(8):
                t_ref[half,k*8+d,0:ROWS,:]=v[ROWS*d:ROWS*d+ROWS]
        return c
    lax.fori_loop(0,16,group,0)
def grad_down(pt,dh):
    return pl.pallas_call(wd_kernel,grid=(D//COLS,),in_specs=[pl.BlockSpec((F,M),lambda n:(0,0)),pl.BlockSpec((M,COLS),lambda n:(0,n))],
        out_specs=pl.BlockSpec((2,LANES,PAD,LANES),lambda n:(n,0,0,0)),out_shape=S((8,LANES,PAD,LANES),f32),
        scratch_shapes=[pltpu.VMEM((F,COLS),f32)],compiler_params=CP(60),cost_estimate=cost(1),name="grad_down")(pt,dh)

def b1_kernel(dh_ref,wd_ref,g_ref,u_ref,at_ref,dg_ref,du_ref,tg_ref,tu_ref,dgs,dus):
    j=pl.program_id(0)
    def front():
        for r in range(0,M,SUB):
            rows=pl.ds(r,SUB)
            dp=dot(dh_ref[rows,:],wd_ref[ALLOF],1,1).astype(bf).astype(f32)
            dg=(dp*g_ref[0,rows,:]).astype(bf)
            du=(dp*u_ref[0,rows,:]).astype(bf)
            dg_ref[0,rows,:]=dg; du_ref[0,rows,:]=du
            dgs[j%2,rows,:]=dg; dus[j%2,rows,:]=du
    def back():
        tg_ref[0]=dot(at_ref[ALLOF],dgs[(j+1)%2])
        tu_ref[0]=dot(at_ref[ALLOF],dus[(j+1)%2])
    @pl.when(j==0)
    def _(): front()
    @pl.when((j>0)&(j<NG))
    def _():
        front(); back()
    @pl.when(j==NG)
    def _(): back()
def grad_gate_up(dh,wd,g,u,at):
    here=lambda j: jnp.minimum(j,NG-1)
    last=lambda j: jnp.maximum(j-1,0)
    blk=pl.BlockSpec((1,M,COLS),lambda j:(here(j),0,0))
    return pl.pallas_call(b1_kernel,grid=(NG+1,),in_specs=[pl.BlockSpec((M,D),lambda j:(0,0)),pl.BlockSpec((COLS,D),lambda j:(here(j),0)),blk,blk,pl.BlockSpec((D,M),lambda j:(0,0))],
        out_specs=[blk]*2+[pl.BlockSpec((1,D,COLS),lambda j:(last(j),0,0))]*2,
        out_shape=[S((NG,M,COLS),bf)]*2+[S((NG,D,COLS),f32)]*2,scratch_shapes=[pltpu.VMEM((2,M,COLS),bf)]*2,
        compiler_params=CP(60),cost_estimate=cost(3),name="grad_gate_up")(dh,wd,g,u,at)

def b2_kernel(dg_ref,du_ref,wg_ref,wu_ref,h_ref,dh_ref,o_ref):
    acc=dot(dg_ref[0],wg_ref[0],1,1)+dot(du_ref[0],wu_ref[0],1,1)
    for j in range(1,NG):
        acc+=dot(dg_ref[j],wg_ref[j],1,1)
        acc+=dot(du_ref[j],wu_ref[j],1,1)
    d=acc.astype(bf).astype(f32)
    h=h_ref[ALLOF].astype(f32)
    scale=lax.rsqrt(jnp.mean(h*h,-1,keepdims=True)+1e-6)
    t=jnp.sum(d*h,-1,keepdims=True)*(scale*scale*scale)*(1.0/D)
    o_ref[ALLOF]=dh_ref[ALLOF]+(d*scale-h*t).astype(bf)
def grad_h(l,dg,du,wg,wu,h,dh):
    row=pl.BlockSpec((BM,D),lambda i:(i,0))
    blk=pl.BlockSpec((NG,BM,COLS),lambda i:(0,i,0))
    w=pl.BlockSpec((NG,D,COLS),lambda i:(l,0,0),pipeline_mode=pl.Buffered(1))
    return pl.pallas_call(b2_kernel,grid=(M//BM,),in_specs=[blk,blk,w,w,row,row],out_specs=row,out_shape=S((M,D),bf),
        compiler_params=CP(60),cost_estimate=cost(2),name="grad_h")(dg,du,wg,wu,h,dh)


def step(x,dy,wg,wu,wd):
    x,dy=x[0],dy[0]
    gg,gu,gd=gather(wg,wu,wd)
    gg,gu=(t.reshape(2*NG,D,COLS) for t in (gg,gu))
    down_w=compact(gd.reshape(16,LANES,PAD,LANES))
    a0,at0=norm(x)
    g0,u0,pt0=gate_up(0,a0,gg,gu)
    h1,a1,at1=down(pt0,down_w[0],x)
    g1,u1,pt1=gate_up(1,a1,gg,gu)
    dh=dy
    terms=[None,None]
    for l,(g,u,pt,at,h) in ((1,(g1,u1,pt1,at1,h1)),(0,(g0,u0,pt0,at0,x))):
        td=grad_down(pt,dh)
        dg,du,tg,tu=grad_gate_up(dh,down_w[l],g,u,at)
        terms[l]=(tg.reshape(NG,RING,RING,RING,2,8,COLS),tu.reshape(NG,RING,RING,RING,2,8,COLS),td.reshape(8,RING,RING,RING,2,PAD,LANES))
        dh=grad_h(l,dg,du,gg,gu,h,dh)
    og,ou,od=reduce_scatter(*zip(*terms,strict=True),2,F,D)
    return dh[None],og,ou,od

def solution(mesh):
    tok=P(("rep","dp"),None,None)
    w=P(None,"dp",None)
    o=P("rep","dp",None)
    return jax.shard_map(step,mesh=mesh,in_specs=(tok,tok,w,w,w),out_specs=(tok,o,o,o),check_vma=False)
```

```python
import functools

import jax
import jax.numpy as jnp
from jax import lax
from jax.experimental import pallas as pl
from jax.experimental.pallas import tpu as pltpu
from jax.sharding import PartitionSpec as P

MESH=pl.DeviceIdType.MESH
bf=jnp.bfloat16
f32=jnp.float32
S=jax.ShapeDtypeStruct
ALLOF=...
ALL=slice(None)
M,D,F,L=2048,1024,2816,2
RING,COLS,LANES=4,256,128
CHIPS=(RING,)*3
TORUS=(*CHIPS,2)
R8,ROWS,PAD,EIGHT=8,22,24,8
GROUP=EIGHT*ROWS
NG,ND=F//COLS,D//LANES
ITEMS=L*NG
BM=256
TILES=M//BM
ORDERS=((2,1,0),(0,2,1),(1,0,2))
HALF_COLS=((pl.ds(0,R8),pl.ds(0,LANES)),(pl.ds(0,R8),pl.ds(LANES,LANES)))
HALF_ROWS=((pl.ds(0,16),pl.ds(0,LANES)),(pl.ds(16,8),pl.ds(0,LANES)))
DMA=pltpu.SemaphoreType.DMA
ANY=pl.BlockSpec(memory_space=pl.ANY)
INVMEM=pl.BlockSpec(memory_space=pltpu.VMEM)
VMEM=pltpu.VMEM

def dot(a,b,ca=1,cb=0):
    return lax.dot_general(a,b,(((ca,),(cb,)),((),())),preferred_element_type=f32)

def rms(h):
    return lax.rsqrt(jnp.mean(h*h,-1,keepdims=True)+1e-6)

def normed(h):
    wide=h.astype(f32)
    return (wide*rms(wide)).astype(bf)

def aligned(i,n):
    return pl.ds(pl.multiple_of(i*n,n),n)

def params(n,mb):
    return pltpu.CompilerParams(collective_id=n,has_side_effects=True,vmem_limit_bytes=mb<<20)


def coords():
    me=lax.axis_index("dp")
    chip=me//2
    return (chip//RING//RING,chip//RING%RING,chip%RING),me%2

def dev(xyz,c):
    return {"dp":((xyz[0]*RING+xyz[1])*RING+xyz[2])*2+c}

def moved(xyz,axis,to):
    return tuple(to if k==axis else v for k,v in enumerate(xyz))

def at(axis,v,axes=(0,1,2)):
    return tuple(v if k==axis else ALL for k in axes)

def sides(xyz,axis,c):
    sigma=1-2*c
    return (xyz[axis]+sigma+RING)%RING,(xyz[axis]-sigma+RING)%RING

def others(xyz,axis):
    return [moved(xyz,axis,(xyz[axis]+d)%RING) for d in range(1,RING)]

def remote(src,dst,sems,slot,k,xyz,c):
    send,recv=sems
    return pltpu.make_async_remote_copy(src_ref=src,dst_ref=dst,send_sem=send.at[slot,k],recv_sem=recv.at[slot,k],
        device_id=dev(xyz,c),device_id_type=MESH)

def entry_barrier():
    xyz,c=coords()
    b=pltpu.get_barrier_semaphore()
    reach=[(to,c) for axis in range(3) for to in others(xyz,axis)]+[(xyz,1-c)]
    for to in reach:
        pl.semaphore_signal(b,inc=1,device_id=dev(*to),device_id_type=MESH)
    pl.semaphore_wait(b,len(reach))


SLOTS=4
G_OFF=(0,2,4,6,8,10,11)
G_DEPTH=G_OFF[-1]
DOWN_STEPS=TILES
F_STEPS=ITEMS+DOWN_STEPS

class Gather:
    def __init__(self,order,g,own,halves,sems,local):
        self.order,self.g,self.own,self.halves,self.sems,self.local=order,g,own,halves,sems,local
    def region(self,item,full,xyz,c,part=(ALL,ALL)):
        return self.g.at[(item,*(ALL if k in full else xyz[k] for k in range(3)),c,*part)]
    def copies(self,stage,item):
        xyz,c=coords()
        a,b,last=self.order
        def copy(k,src,dst,to,tc=c):
            return remote(src,dst,self.sems,item%SLOTS,k,to,tc)
        if stage==0:
            mine=self.region(item,(),xyz,c)
            return [copy(k,self.own(item),mine,to) for k,to in enumerate(others(xyz,a))]
        if stage==5:
            mine=self.region(item,(0,1,2),xyz,c)
            return [copy(11,mine,mine,xyz,1-c)]
        axis,full,k=(b,(a,),3) if stage<3 else (last,(a,b),7)
        p,q=sides(xyz,axis,c)
        if stage%2:
            mine=self.region(item,full,xyz,c)
            return [copy(k,mine,mine,moved(xyz,axis,p)),copy(k+1,mine,mine,moved(xyz,axis,q))]
        fromq=self.region(item,full,moved(xyz,axis,q),c,self.halves[0])
        fromp=self.region(item,full,moved(xyz,axis,p),c,self.halves[1])
        return [copy(k+2,fromq,fromq,moved(xyz,axis,p)),copy(k+3,fromp,fromp,moved(xyz,axis,q))]
    def own_copy(self,item):
        xyz,c=coords()
        return pltpu.make_async_copy(self.own(item),self.region(item,(),xyz,c),self.local.at[item%SLOTS])
    def run(self,stage,item):
        if stage>0:
            for cp in self.copies(stage-1,item): cp.wait()
            if stage==1: self.own_copy(item).wait()
        if stage<6:
            for cp in self.copies(stage,item): cp.start()
            if stage==0: self.own_copy(item).start()

def f_kernel(x,wg,wu,wd,gg,gu,gd,ga,gb,pt,at_,h1,wc,
        wdp,xv,av,ptv,wcv,wv,dv,abv,atv,hv,xsem,wsem,dsem,absem,ptsem,atsem,hsem,wcsem,*gsems):
    for l in range(L):
        wdp[l,0:ROWS,:]=wd[l]
        wdp[l,ROWS:PAD,:]=jnp.zeros((PAD-ROWS,D),bf)
    load_x=pltpu.make_async_copy(x,xv,xsem)
    load_x.start()
    entry_barrier()
    own_g=lambda i: wg.at[i//NG,:,aligned(i%NG,COLS)]
    own_u=lambda i: wu.at[i//NG,:,aligned(i%NG,COLS)]
    own_d=lambda k: wdp.at[k//ND,:,aligned(k%ND,LANES)]
    eg=Gather(ORDERS[0],gg,own_g,HALF_COLS,gsems[0:2],gsems[2])
    eu=Gather(ORDERS[1],gu,own_u,HALF_COLS,gsems[3:5],gsems[5])
    ed=Gather(ORDERS[2],gd,own_d,HALF_ROWS,gsems[6:8],gsems[8])
    down_of=lambda i: i//NG*ND+i%NG
    def load_d(k):
        return pltpu.make_async_copy(gd.at[k],dv.at[k%2],dsem.at[k%2])
    def store_wc(l):
        return pltpu.make_async_copy(wcv.at[l],wc.at[l],wcsem.at[l])
    def compact(k):
        load_d(k).wait()
        def group(j,carry):
            v=dv[k%2,j//RING,j%RING].reshape(EIGHT,PAD,LANES).astype(f32)
            wcv[k//ND,aligned(j,GROUP),aligned(k%ND,LANES)]=jnp.concatenate([v[d,0:ROWS] for d in range(EIGHT)],0).astype(bf)
            return carry
        lax.fori_loop(0,16,group,0)
        @pl.when(k%ND==ND-1)
        def _(): store_wc(k//ND).start()
    def tick(t):
        i=t-G_DEPTH-1
        @pl.when((i>=0)&(i<ITEMS)&(i%NG<ND))
        def _(): compact(down_of(i))
        for stage in reversed(range(7)):
            i=t-G_OFF[stage]
            @pl.when((i>=0)&(i<ITEMS))
            def _():
                eg.run(stage,i); eu.run(stage,i)
                @pl.when(i%NG<ND)
                def _():
                    ed.run(stage,down_of(i))
                    if stage==6: load_d(down_of(i)).start()
    item_of=lambda k: jnp.where(k<NG,k,k-DOWN_STEPS)
    is_item=lambda k: ((k>=0)&(k<NG))|((k>=NG+DOWN_STEPS)&(k<F_STEPS))
    def load_w(i):
        return [pltpu.make_async_copy(g.at[i],wv.at[m,i%2],wsem.at[m,i%2]) for m,g in enumerate((gg,gu))]
    def store_ab(i):
        s=i%2
        return [pltpu.make_async_copy(abv.at[m,s],o.at[i//NG,i%NG],absem.at[m,s]) for m,o in enumerate((ga,gb))]+[
            pltpu.make_async_copy(ptv.at[aligned(i%NG,COLS)],pt.at[i//NG,aligned(i%NG,COLS)],ptsem.at[s])]
    def store_at(l,r):
        return pltpu.make_async_copy(atv.at[r%2],at_.at[l,:,aligned(r,BM)],atsem.at[r%2])
    def store_h(r):
        return pltpu.make_async_copy(hv.at[r%2],h1.at[aligned(r,BM)],hsem.at[r%2])
    def put_a(l,r,h):
        a=normed(h)
        av[aligned(r,BM),:]=a
        @pl.when(r>=2)
        def _(): store_at(l,r-2).wait()
        atv[r%2]=a.T
        store_at(l,r).start()
    def gate_up(i):
        for cp in load_w(i): cp.wait()
        @pl.when(i>=2)
        def _():
            for cp in store_ab(i-2): cp.wait()
        s=i%2
        w_gate,w_up=(wv[m,s].reshape(D,COLS) for m in range(2))
        for r in range(TILES):
            rows=pl.ds(r*BM,BM)
            g=dot(av[rows,:],w_gate)
            u=dot(av[rows,:],w_up)
            sg=jax.nn.sigmoid(g)
            b=g*sg
            abv[0,s,rows,:]=u*(sg+b*(1-sg))
            abv[1,s,rows,:]=b
            ptv[aligned(i%NG,COLS),rows]=(b*u).astype(bf).T
        for cp in store_ab(i): cp.start()
    def down(r):
        y=dot(ptv[:,aligned(r,BM)],wcv[0],0,0).astype(bf)
        h=xv[aligned(r,BM),:]+y
        @pl.when(r>=2)
        def _(): store_h(r-2).wait()
        hv[r%2]=h
        store_h(r).start()
        put_a(1,r,h)
    tick(0)
    load_x.wait()
    def norm(r,carry):
        put_a(0,r,xv[aligned(r,BM),:])
        return carry
    lax.fori_loop(0,TILES,norm,0)
    for r in (TILES-2,TILES-1): store_at(0,r).wait()
    def step(t,carry):
        k=t-G_DEPTH-1
        tick(t)
        @pl.when(is_item(k+1))
        def _():
            for cp in load_w(item_of(k+1)): cp.start()
        @pl.when(is_item(k))
        def _(): gate_up(item_of(k))
        @pl.when((k>=NG)&(k<NG+DOWN_STEPS))
        def _(): down(k-NG)
        return carry
    lax.fori_loop(1,F_STEPS+G_DEPTH+1,step,0)
    for r in (TILES-2,TILES-1):
        store_at(1,r).wait()
        store_h(r).wait()
    for i in (ITEMS-2,ITEMS-1):
        for cp in store_ab(i): cp.wait()
    for l in range(L): store_wc(l).wait()

def forward(x,wg,wu,wd):
    return pl.pallas_call(f_kernel,
        out_shape=[S((ITEMS,*TORUS,R8,COLS),bf)]*2+[S((L*ND,*TORUS,PAD,LANES),bf)]+[S((L,NG,M,COLS),f32)]*2+[
            S((L,F,M),bf),S((L,D,M),bf),S((M,D),bf),S((L,F,D),bf)],
        in_specs=[ANY]+[INVMEM]*3,out_specs=[ANY]*9,
        scratch_shapes=[VMEM((L,PAD,D),bf),VMEM((M,D),bf),VMEM((M,D),bf),VMEM((F,M),bf),VMEM((L,F,D),bf),VMEM((2,2,*TORUS,R8,COLS),bf),
            VMEM((2,*TORUS,PAD,LANES),bf),VMEM((2,2,M,COLS),f32),VMEM((2,D,BM),bf),VMEM((2,BM,D),bf),
            DMA,DMA((2,2)),DMA((2,)),DMA((2,2)),DMA((2,)),DMA((2,)),DMA((2,)),DMA((L,))]+[DMA((SLOTS,12)),DMA((SLOTS,12)),DMA((SLOTS,))]*3,
        compiler_params=params(0,62),name="forward")(x,wg,wu,wd)

HC=HALF_COLS
HR=HALF_ROWS
CP=lambda mb: pltpu.CompilerParams(vmem_limit_bytes=mb<<20)
def cost(n): return pl.CostEstimate(flops=2*M*D*F*n,bytes_accessed=1<<24,transcendentals=0)
SUB=256
class Scatter:
    STAGES=7
    TW=RING
    @staticmethod
    def scratch(R,n,halves):
        (ra,ca),(rb,cb)=halves
        V=lambda *s: pltpu.VMEM(s,bf)
        return dict(ds=V(2,RING,RING,RING,R,n),dr=V(RING,RING,RING,RING,R,n),
            a1s=V(2,RING,RING,R,n),a1A=V(2,RING,RING,ra.size,ca.size),a1B=V(2,RING,RING,rb.size,cb.size),
            a2s=V(2,2,RING,RING,R,n),a2r=V(2,2,RING,RING,R,n),t1=pltpu.VMEM((2,RING,RING,R,n),f32),
            b1s=V(2,RING,R,n),b1A=V(2,RING,ra.size,ca.size),b1B=V(2,RING,rb.size,cb.size),
            b2s=V(2,2,RING,R,n),b2r=V(2,2,RING,R,n),t2=pltpu.VMEM((2,RING,R,n),f32),
            cs=V(2,3,R,n),cr=V(2,3,R,n),
            send=pltpu.SemaphoreType.DMA((2,12)),recv=pltpu.SemaphoreType.DMA((2,12)))
    def __init__(self,order,term,out,halves,refs):
        self.order,self.term,self.out,self.halves=order,term,out,halves
        self.__dict__.update(refs)
    def geometry(self):
        xyz,c=coords()
        cx,b,a=self.order
        sigma=1-2*c
        return xyz,c,a,b,cx,sigma
    def copies(self,stage,item):
        xyz,c,a,b,cx,sigma=self.geometry()
        s=item%2
        def copy(k,src,dst,to,tc=None):
            return pltpu.make_async_remote_copy(src_ref=src,dst_ref=dst,send_sem=self.send.at[s,k],recv_sem=self.recv.at[s,k],
                device_id=dev(to,c if tc is None else tc),device_id_type=MESH)
        if stage==0: return [copy(0,self.ds.at[s],self.dr.at[item%RING],xyz,1-c)]
        if stage in (1,3):
            axis=a if stage==1 else b
            k,src,A,B=(1,self.a1s,self.a1A,self.a1B) if stage==1 else (5,self.b1s,self.b1A,self.b1B)
            lead=(ALL,)*(2 if stage==1 else 1)
            p,q=(xyz[axis]+sigma+RING)%RING,(xyz[axis]-sigma+RING)%RING
            (ra,ca),(rb,cb)=self.halves
            return [copy(k,src.at[(s,*lead,ra,ca)],A.at[s],moved(xyz,axis,p)),copy(k+1,src.at[(s,*lead,rb,cb)],B.at[s],moved(xyz,axis,q))]
        if stage in (2,RING):
            axis=a if stage==2 else b
            k,src,dst=(3,self.a2s,self.a2r) if stage==2 else (7,self.b2s,self.b2r)
            p,q=(xyz[axis]+sigma+RING)%RING,(xyz[axis]-sigma+RING)%RING
            return [copy(k,src.at[s,0],dst.at[s,0],moved(xyz,axis,p)),copy(k+1,src.at[s,1],dst.at[s,1],moved(xyz,axis,q))]
        if stage==5:
            return [copy(8+d,self.cs.at[s,d-1],self.cr.at[s,d-1],moved(xyz,cx,(xyz[cx]+d)%RING)) for d in (1,2,3)]
    def run(self,stage,item):
        xyz,c,a,b,cx,sigma=self.geometry()
        s=item%2
        ts=item%self.TW; d4=item%RING
        (ra,ca),(rb,cb)=self.halves
        if stage>0:
            for cp in self.copies(stage-1,item): cp.wait()
        def plane(v):
            ix=tuple(v if k==a else ALL for k in range(3))
            return self.term[(ts,*ix,c)]+self.dr[(d4,*ix)].astype(f32)
        rem=[k for k in range(3) if k!=a]
        def line(v):
            ix=tuple(v if k==b else ALL for k in rem)
            return self.t1[(s,*ix)]
        if stage==0:
            self.ds[s]=self.term[ts,:,:,:,1-c].astype(bf)
        elif stage in (1,3):
            if stage==3:
                self.t1[s]=plane(xyz[a])+self.a2r[s,0].astype(f32)+self.a2r[s,1].astype(f32)
            axis,get,dst=(a,plane,self.a1s) if stage==1 else (b,line,self.b1s)
            dst[s]=get((xyz[axis]+2)%RING).astype(bf)
        elif stage in (2,RING):
            axis,get,dst,A,B,nd=(a,plane,self.a2s,self.a1A,self.a1B,2) if stage==2 else (b,line,self.b2s,self.b1A,self.b1B,1)
            lead=(ALL,)*nd
            p,q=(xyz[axis]+sigma+RING)%RING,(xyz[axis]-sigma+RING)%RING
            vp,vq=get(p),get(q)
            st=lambda k,r,cl,v: dst.__setitem__((s,k,*lead,r,cl),v.astype(bf))
            cut=lambda v,r,cl: v[(*lead,slice(r.start,r.start+r.size),slice(cl.start,cl.start+cl.size))]
            st(0,ra,ca,cut(vp,ra,ca)+A[s].astype(f32)); st(0,rb,cb,cut(vp,rb,cb))
            st(1,ra,ca,cut(vq,ra,ca)); st(1,rb,cb,cut(vq,rb,cb)+B[s].astype(f32))
        elif stage==5:
            self.t2[s]=line(xyz[b])+self.b2r[s,0].astype(f32)+self.b2r[s,1].astype(f32)
            for d in (1,2,3):
                self.cs[s,d-1]=self.t2[s,(xyz[cx]+d)%RING].astype(bf)
        else:
            v=self.t2[s,xyz[cx]]
            for d in range(3): v=v+self.cr[s,d].astype(f32)
            self.out(item,v.astype(bf))
        if stage<6:
            for cp in self.copies(stage,item): cp.start()

HC=((pl.ds(0,8),pl.ds(0,LANES)),(pl.ds(0,8),pl.ds(LANES,LANES)))
HR=((pl.ds(0,16),pl.ds(0,LANES)),(pl.ds(16,8),pl.ds(0,LANES)))

def rs_kernel(L,ng,nd,tg0,tg1,tu0,tu1,td0,td1,og,ou,od,odp,vg,vu,vd,lsem,*scr):
    n1=len(Scatter.scratch(8,COLS,HC))
    keys=list(Scatter.scratch(8,COLS,HC))
    pack=lambda k: dict(zip(keys,scr[k*n1:(k+1)*n1],strict=True))
    entry_barrier()
    items=L*ng
    lay=lambda i: L-1-i//ng
    idx=lambda i: lay(i)*ng+i%ng
    cols=lambda i: pl.ds(pl.multiple_of(i%ng*COLS,COLS),COLS)
    def outg(i,v): og[lay(i),:,cols(i)]=v
    def outu(i,v): ou[lay(i),:,cols(i)]=v
    def outd(k,v): odp[L-1-k//nd,:,pl.ds(pl.multiple_of(k%nd*LANES,LANES),LANES)]=v
    eg=Scatter(ORDERS[0],vg,outg,HC,pack(0))
    eu=Scatter(ORDERS[1],vu,outu,HC,pack(1))
    ed=Scatter(ORDERS[2],vd,outd,HR,pack(2))
    dk=lambda i: i//ng*nd+i%ng
    didx=lambda k: (L-1-k//nd)*nd+k%nd
    def load(m,i,go):
        v=(vg,vu,vd)[m]
        k,slot=(i%ng,i%RING) if m<2 else (i%ng,dk(i)%RING)
        for l,src in enumerate(((tg0,tg1),(tu0,tu1),(td0,td1))[m]):
            @pl.when(lay(i)==l)
            def _():
                cp=pltpu.make_async_copy(src.at[k],v.at[slot],lsem.at[m,i%2])
                cp.start() if go else cp.wait()
    def loads(i,go):
        load(0,i,go); load(1,i,go)
        @pl.when(i%ng<nd)
        def _(): load(2,i,go)
    loads(0,True)
    def tick(t,carry):
        for stage in reversed(range(7)):
            i=t-stage
            @pl.when((i>=0)&(i<items))
            def _():
                if stage==0: loads(i,False)
                eg.run(stage,i); eu.run(stage,i)
                @pl.when(i%ng<nd)
                def _(): ed.run(stage,dk(i))
        @pl.when(t+1<items)
        def _(): loads(t+1,True)
        return carry
    lax.fori_loop(0,items+6,tick,0)
    od[ALLOF]=odp[:,0:ROWS,:]

def reduce_scatter(tg,tu,td,L,F,D):
    ng,nd=F//COLS,D//LANES
    def flat(R,n,h): return list(Scatter.scratch(R,n,h).values())
    f=pl.pallas_call(functools.partial(rs_kernel,L,ng,nd),
        out_shape=[jax.ShapeDtypeStruct((L,8,F),bf)]*2+[jax.ShapeDtypeStruct((L,ROWS,D),bf)],
        in_specs=[pl.BlockSpec(memory_space=pl.ANY)]*6,
        out_specs=[pl.BlockSpec(memory_space=pltpu.VMEM)]*3,
        scratch_shapes=[pltpu.VMEM((L,PAD,D),bf),pltpu.VMEM((RING,RING,RING,RING,2,8,COLS),f32),pltpu.VMEM((RING,RING,RING,RING,2,8,COLS),f32),pltpu.VMEM((RING,RING,RING,RING,2,PAD,LANES),f32),
            pltpu.SemaphoreType.DMA((3,2))]+flat(8,COLS,HC)*2+flat(PAD,LANES,HR),
        compiler_params=pltpu.CompilerParams(collective_id=1,has_side_effects=True,vmem_limit_bytes=60<<20),name="scatter")
    return tuple(f(*tg,*tu,*td))

def wd_kernel(pt_ref,dh_ref,t_ref,acc):
    acc[ALLOF]=dot(pt_ref[ALLOF],dh_ref[ALLOF])
    def group(k,c):
        for half in range(2):
            v=acc[pl.ds(pl.multiple_of(k*GROUP,GROUP),GROUP),pl.ds(half*LANES,LANES)]
            for d in range(8):
                t_ref[half,k*8+d,0:ROWS,:]=v[ROWS*d:ROWS*d+ROWS]
        return c
    lax.fori_loop(0,16,group,0)
def grad_down(pt,dh):
    return pl.pallas_call(wd_kernel,grid=(D//COLS,),in_specs=[pl.BlockSpec((F,M),lambda n:(0,0)),pl.BlockSpec((M,COLS),lambda n:(0,n))],
        out_specs=pl.BlockSpec((2,LANES,PAD,LANES),lambda n:(n,0,0,0)),out_shape=S((8,LANES,PAD,LANES),f32),
        scratch_shapes=[pltpu.VMEM((F,COLS),f32)],compiler_params=CP(60),cost_estimate=cost(1),name="grad_down")(pt,dh)

def b1_kernel(dh_ref,wd_ref,g_ref,u_ref,at_ref,dg_ref,du_ref,tg_ref,tu_ref,dgs,dus):
    j=pl.program_id(0)
    def front():
        for r in range(0,M,SUB):
            rows=pl.ds(r,SUB)
            dp=dot(dh_ref[rows,:],wd_ref[ALLOF],1,1).astype(bf).astype(f32)
            dg=(dp*g_ref[0,rows,:]).astype(bf)
            du=(dp*u_ref[0,rows,:]).astype(bf)
            dg_ref[0,rows,:]=dg; du_ref[0,rows,:]=du
            dgs[j%2,rows,:]=dg; dus[j%2,rows,:]=du
    def back():
        tg_ref[0]=dot(at_ref[ALLOF],dgs[(j+1)%2])
        tu_ref[0]=dot(at_ref[ALLOF],dus[(j+1)%2])
    @pl.when(j==0)
    def _(): front()
    @pl.when((j>0)&(j<NG))
    def _():
        front(); back()
    @pl.when(j==NG)
    def _(): back()
def grad_gate_up(dh,wd,g,u,at):
    here=lambda j: jnp.minimum(j,NG-1)
    last=lambda j: jnp.maximum(j-1,0)
    blk=pl.BlockSpec((1,M,COLS),lambda j:(here(j),0,0))
    return pl.pallas_call(b1_kernel,grid=(NG+1,),in_specs=[pl.BlockSpec((M,D),lambda j:(0,0)),pl.BlockSpec((COLS,D),lambda j:(here(j),0)),blk,blk,pl.BlockSpec((D,M),lambda j:(0,0))],
        out_specs=[blk]*2+[pl.BlockSpec((1,D,COLS),lambda j:(last(j),0,0))]*2,
        out_shape=[S((NG,M,COLS),bf)]*2+[S((NG,D,COLS),f32)]*2,scratch_shapes=[pltpu.VMEM((2,M,COLS),bf)]*2,
        compiler_params=CP(60),cost_estimate=cost(3),name="grad_gate_up")(dh,wd,g,u,at)

def b2_kernel(dg_ref,du_ref,wg_ref,wu_ref,h_ref,dh_ref,o_ref):
    acc=dot(dg_ref[0],wg_ref[0],1,1)+dot(du_ref[0],wu_ref[0],1,1)
    for j in range(1,NG):
        acc+=dot(dg_ref[j],wg_ref[j],1,1)
        acc+=dot(du_ref[j],wu_ref[j],1,1)
    d=acc.astype(bf).astype(f32)
    h=h_ref[ALLOF].astype(f32)
    scale=lax.rsqrt(jnp.mean(h*h,-1,keepdims=True)+1e-6)
    t=jnp.sum(d*h,-1,keepdims=True)*(scale*scale*scale)*(1.0/D)
    o_ref[ALLOF]=dh_ref[ALLOF]+(d*scale-h*t).astype(bf)
def grad_h(l,dg,du,wg,wu,h,dh):
    row=pl.BlockSpec((BM,D),lambda i:(i,0))
    blk=pl.BlockSpec((NG,BM,COLS),lambda i:(0,i,0))
    w=pl.BlockSpec((NG,D,COLS),lambda i:(l,0,0),pipeline_mode=pl.Buffered(1))
    return pl.pallas_call(b2_kernel,grid=(M//BM,),in_specs=[blk,blk,w,w,row,row],out_specs=row,out_shape=S((M,D),bf),
        compiler_params=CP(60),cost_estimate=cost(2),name="grad_h")(dg,du,wg,wu,h,dh)


def step(x,dy,wg,wu,wd):
    x,dy=x[0],dy[0]
    gg,gu,_,ga,gb,pt,at_,h1,wc=forward(x,wg,wu,wd)
    gg,gu=(t.reshape(2*NG,D,256) for t in (gg,gu))
    dh=dy
    terms=[None,None]
    for l,h in ((1,h1),(0,x)):
        td=grad_down(pt[l],dh)
        dg,du,tg,tu=grad_gate_up(dh,wc[l],ga[l],gb[l],at_[l])
        terms[l]=(tg.reshape(NG,4,4,4,2,8,256),tu.reshape(NG,4,4,4,2,8,256),td.reshape(8,4,4,4,2,24,128))
        dh=grad_h(l,dg,du,gg,gu,h,dh)
    og,ou,od=reduce_scatter(*zip(*terms,strict=True),2,F,D)
    return dh[None],og,ou,od

def solution(mesh):
    tok=P(("rep","dp"),None,None)
    w=P(None,"dp",None)
    o=P("rep","dp",None)
    return jax.shard_map(step,mesh=mesh,in_specs=(tok,tok,w,w,w),out_specs=(tok,o,o,o),check_vma=False)
```

```python
import functools

import jax
import jax.numpy as jnp
from jax import lax
from jax.experimental import pallas as pl
from jax.experimental.pallas import tpu as pltpu
from jax.sharding import PartitionSpec as P

MESH=pl.DeviceIdType.MESH
bf=jnp.bfloat16
f32=jnp.float32
S=jax.ShapeDtypeStruct
ALLOF=...
ALL=slice(None)
M,D,F,L=2048,1024,2816,2
RING,COLS,LANES=4,256,128
CHIPS=(RING,)*3
TORUS=(*CHIPS,2)
R8,ROWS,PAD,EIGHT=8,22,24,8
GROUP=EIGHT*ROWS
NG,ND=F//COLS,D//LANES
ITEMS=L*NG
BM=256
TILES=M//BM
ORDERS=((2,1,0),(0,2,1),(1,0,2))
HALF_COLS=((pl.ds(0,R8),pl.ds(0,LANES)),(pl.ds(0,R8),pl.ds(LANES,LANES)))
HALF_ROWS=((pl.ds(0,16),pl.ds(0,LANES)),(pl.ds(16,8),pl.ds(0,LANES)))
DMA=pltpu.SemaphoreType.DMA
ANY=pl.BlockSpec(memory_space=pl.ANY)
INVMEM=pl.BlockSpec(memory_space=pltpu.VMEM)
VMEM=pltpu.VMEM

def dot(a,b,ca=1,cb=0):
    return lax.dot_general(a,b,(((ca,),(cb,)),((),())),preferred_element_type=f32)

def rms(h):
    return lax.rsqrt(jnp.mean(h*h,-1,keepdims=True)+1e-6)

def normed(h):
    wide=h.astype(f32)
    return (wide*rms(wide)).astype(bf)

def aligned(i,n):
    return pl.ds(pl.multiple_of(i*n,n),n)

def params(n,mb):
    return pltpu.CompilerParams(collective_id=n,has_side_effects=True,vmem_limit_bytes=mb<<20)


class Torus:
    def __init__(self):
        me=lax.axis_index("dp")
        chip,self.c=lax.div(me,2),lax.rem(me,2)
        self.xyz=(lax.div(chip,RING*RING),lax.rem(lax.div(chip,RING),RING),lax.rem(chip,RING))
        self.partner=me+1-2*self.c
        weight=(2*RING*RING,2*RING,2)
        sigma=1-2*self.c
        self.ring,self.ringid,self.p,self.q,self.pid,self.qid=[],[],[],[],[],[]
        for v,w in zip(self.xyz,weight,strict=True):
            place=lambda d: lax.rem(v+d,RING)
            ident=lambda u: me+(u-v)*w
            ring=[place(d) for d in range(1,RING)]
            p,q=place(RING+sigma),place(RING-sigma)
            for to,value in ((self.ring,ring),(self.ringid,[ident(u) for u in ring]),(self.p,p),(self.q,q),(self.pid,ident(p)),(self.qid,ident(q))):
                to.append(value)

    def barrier(self):
        b=pltpu.get_barrier_semaphore()
        reach=[to for ids in self.ringid for to in ids]+[self.partner]
        for to in reach:
            pl.semaphore_signal(b,inc=1,device_id={"dp":to},device_id_type=MESH)
        pl.semaphore_wait(b,len(reach))

def at(axis,v,axes=(0,1,2)):
    return tuple(v if k==axis else ALL for k in axes)

def remote(src,dst,sems,slot,k,to):
    send,recv=sems
    return pltpu.make_async_remote_copy(src_ref=src,dst_ref=dst,send_sem=send.at[slot,k],recv_sem=recv.at[slot,k],
        device_id={"dp":to},device_id_type=MESH)


SLOTS=4
G_OFF=(0,2,4,6,8,10,11)
G_DEPTH=G_OFF[-1]
DOWN_STEPS=TILES
F_STEPS=ITEMS+DOWN_STEPS

class Gather:
    def __init__(self,torus,order,g,own,halves,sems,local):
        self.t,self.order,self.g,self.own,self.halves,self.sems,self.local=torus,order,g,own,halves,sems,local
    def region(self,i,full,axis=None,v=None,part=(ALL,ALL)):
        where=(ALL if k in full else v if k==axis else self.t.xyz[k] for k in range(3))
        return self.g.at[(i,*where,self.t.c,*part)]
    def copies(self,stage,i):
        t=self.t
        a,b,last=self.order
        copy=lambda k,src,dst,to: remote(src,dst,self.sems,lax.rem(i,SLOTS),k,to)
        if stage==0:
            mine=self.region(i,())
            return [copy(k,self.own(i),mine,to) for k,to in enumerate(t.ringid[a])]
        if stage==5:
            mine=self.region(i,(0,1,2))
            return [copy(11,mine,mine,t.partner)]
        axis,full,k=(b,(a,),3) if stage<3 else (last,(a,b),7)
        to=(t.pid[axis],t.qid[axis])
        if stage%2:
            mine=self.region(i,full)
            return [copy(k+d,mine,mine,to[d]) for d in range(2)]
        came=(t.q[axis],t.p[axis])
        parts=[self.region(i,full,axis,came[d],self.halves[d]) for d in range(2)]
        return [copy(k+2+d,parts[d],parts[d],to[d]) for d in range(2)]
    def own_copy(self,i):
        return pltpu.make_async_copy(self.own(i),self.region(i,()),self.local.at[lax.rem(i,SLOTS)])
    def run(self,stage,i):
        if stage>0:
            for cp in self.copies(stage-1,i): cp.wait()
            if stage==1: self.own_copy(i).wait()
        if stage<6:
            for cp in self.copies(stage,i): cp.start()
            if stage==0: self.own_copy(i).start()

def f_kernel(x,wg,wu,wd,gg,gu,gd,ga,gb,pt,at_,h1,wc,
        wdp,xv,av,ptv,wcv,wv,dv,abv,atv,hv,xsem,wsem,dsem,absem,ptsem,atsem,hsem,wcsem,*gsems):
    for l in range(L):
        wdp[l,0:ROWS,:]=wd[l]
        wdp[l,ROWS:PAD,:]=jnp.zeros((PAD-ROWS,D),bf)
    load_x=pltpu.make_async_copy(x,xv,xsem)
    load_x.start()
    torus=Torus()
    torus.barrier()
    own_g=lambda i: wg.at[lax.div(i,NG),:,aligned(lax.rem(i,NG),COLS)]
    own_u=lambda i: wu.at[lax.div(i,NG),:,aligned(lax.rem(i,NG),COLS)]
    own_d=lambda k: wdp.at[lax.div(k,ND),:,aligned(lax.rem(k,ND),LANES)]
    eg=Gather(torus,ORDERS[0],gg,own_g,HALF_COLS,gsems[0:2],gsems[2])
    eu=Gather(torus,ORDERS[1],gu,own_u,HALF_COLS,gsems[3:5],gsems[5])
    ed=Gather(torus,ORDERS[2],gd,own_d,HALF_ROWS,gsems[6:8],gsems[8])
    def load_d(k):
        return pltpu.make_async_copy(gd.at[k],dv.at[lax.rem(k,2)],dsem.at[lax.rem(k,2)])
    def store_wc(l):
        return pltpu.make_async_copy(wcv.at[l],wc.at[l],wcsem.at[l])
    def compact(k):
        load_d(k).wait()
        def group(j,carry):
            v=dv[lax.rem(k,2),lax.div(j,RING),lax.rem(j,RING)].reshape(EIGHT,PAD,LANES).astype(f32)
            wcv[lax.div(k,ND),aligned(j,GROUP),aligned(lax.rem(k,ND),LANES)]=jnp.concatenate([v[d,0:ROWS] for d in range(EIGHT)],0).astype(bf)
            return carry
        lax.fori_loop(0,16,group,0)
        @pl.when(lax.rem(k,ND)==ND-1)
        def _(): store_wc(lax.div(k,ND)).start()
    def tick(t):
        i=t-G_DEPTH-1
        @pl.when((i>=0)&(i<L*ND))
        def _(): compact(i)
        for stage in reversed(range(7)):
            i=t-G_OFF[stage]
            @pl.when((i>=0)&(i<ITEMS))
            def _():
                eg.run(stage,i); eu.run(stage,i)
                @pl.when(i<L*ND)
                def _():
                    ed.run(stage,i)
                    if stage==6: load_d(i).start()
    item_of=lambda k: jnp.where(k<NG,k,k-DOWN_STEPS)
    is_item=lambda k: ((k>=0)&(k<NG))|((k>=NG+DOWN_STEPS)&(k<F_STEPS))
    def load_w(i):
        return [pltpu.make_async_copy(g.at[i],wv.at[m,lax.rem(i,2)],wsem.at[m,lax.rem(i,2)]) for m,g in enumerate((gg,gu))]
    def store_ab(i):
        s=lax.rem(i,2)
        return [pltpu.make_async_copy(abv.at[m,s],o.at[lax.div(i,NG),lax.rem(i,NG)],absem.at[m,s]) for m,o in enumerate((ga,gb))]+[
            pltpu.make_async_copy(ptv.at[:,aligned(lax.rem(i,NG),COLS)],pt.at[lax.div(i,NG),:,aligned(lax.rem(i,NG),COLS)],ptsem.at[s])]
    def store_at(l,r):
        return pltpu.make_async_copy(atv.at[lax.rem(r,2)],at_.at[l,:,aligned(r,BM)],atsem.at[lax.rem(r,2)])
    def store_h(r):
        return pltpu.make_async_copy(hv.at[lax.rem(r,2)],h1.at[aligned(r,BM)],hsem.at[lax.rem(r,2)])
    def put_a(l,r,h):
        a=normed(h)
        av[aligned(r,BM),:]=a
        @pl.when(r>=2)
        def _(): store_at(l,r-2).wait()
        atv[lax.rem(r,2)]=a.T
        store_at(l,r).start()
    def gate_up(i):
        for cp in load_w(i): cp.wait()
        @pl.when(i>=2)
        def _():
            for cp in store_ab(i-2): cp.wait()
        s=lax.rem(i,2)
        w_gate,w_up=(wv[m,s].reshape(D,COLS) for m in range(2))
        for r in range(TILES):
            rows=pl.ds(r*BM,BM)
            g=dot(av[rows,:],w_gate)
            u=dot(av[rows,:],w_up)
            sg=jax.nn.sigmoid(g)
            b=g*sg
            abv[0,s,rows,:]=u*(sg+b*(1-sg))
            abv[1,s,rows,:]=b
            ptv[r,aligned(lax.rem(i,NG),COLS),:]=(b*u).astype(bf).T
        for cp in store_ab(i): cp.start()
    def down(r):
        y=dot(ptv[r],wcv[0],0,0).astype(bf)
        h=xv[aligned(r,BM),:]+y
        @pl.when(r>=2)
        def _(): store_h(r-2).wait()
        hv[lax.rem(r,2)]=h
        store_h(r).start()
        put_a(1,r,h)
    tick(0)
    load_x.wait()
    def norm(r,carry):
        put_a(0,r,xv[aligned(r,BM),:])
        return carry
    lax.fori_loop(0,TILES,norm,0)
    for r in (TILES-2,TILES-1): store_at(0,r).wait()
    def step(t,carry):
        k=t-G_DEPTH-1
        tick(t)
        @pl.when(is_item(k+1))
        def _():
            for cp in load_w(item_of(k+1)): cp.start()
        @pl.when(is_item(k))
        def _(): gate_up(item_of(k))
        @pl.when((k>=NG)&(k<NG+DOWN_STEPS))
        def _(): down(k-NG)
        return carry
    lax.fori_loop(1,F_STEPS+G_DEPTH+1,step,0)
    for r in (TILES-2,TILES-1):
        store_at(1,r).wait()
        store_h(r).wait()
    for i in (ITEMS-2,ITEMS-1):
        for cp in store_ab(i): cp.wait()
    for l in range(L): store_wc(l).wait()

def forward(x,wg,wu,wd):
    return pl.pallas_call(f_kernel,
        out_shape=[S((ITEMS,*TORUS,R8,COLS),bf)]*2+[S((L*ND,*TORUS,PAD,LANES),bf)]+[S((L,NG,M,COLS),f32)]*2+[
            S((L,TILES,F,BM),bf),S((L,D,M),bf),S((M,D),bf),S((L,F,D),bf)],
        in_specs=[ANY]+[INVMEM]*3,out_specs=[ANY]*9,
        scratch_shapes=[VMEM((L,PAD,D),bf),VMEM((M,D),bf),VMEM((M,D),bf),VMEM((TILES,F,BM),bf),VMEM((L,F,D),bf),VMEM((2,2,*TORUS,R8,COLS),bf),
            VMEM((2,*TORUS,PAD,LANES),bf),VMEM((2,2,M,COLS),f32),VMEM((2,D,BM),bf),VMEM((2,BM,D),bf),
            DMA,DMA((2,2)),DMA((2,)),DMA((2,2)),DMA((2,)),DMA((2,)),DMA((2,)),DMA((L,))]+[DMA((SLOTS,12)),DMA((SLOTS,12)),DMA((SLOTS,))]*3,
        compiler_params=params(0,62),name="forward")(x,wg,wu,wd)


B_TAIL=NG+1
B_STEPS=B_TAIL+TILES
SEND,DOWN=2,2
S_STAGES=7

class Scatter:
    @staticmethod
    def scratch(rows,n,halves,own=4,ds=2):
        V=lambda *s: VMEM((2,*s),bf)
        A,B=((r.size,c.size) for r,c in halves)
        plane,line=(RING,RING),(RING,)
        return [VMEM((own,*CHIPS,rows,n),f32),VMEM((ds,*CHIPS,rows,n),bf),V(*CHIPS,rows,n),
            V(*plane,rows,n),V(*plane,*A),V(*plane,*B),V(2,*plane,rows,n),V(2,*plane,rows,n),VMEM((2,*plane,rows,n),f32),
            V(*line,rows,n),V(*line,*A),V(*line,*B),V(2,*line,rows,n),V(2,*line,rows,n),VMEM((2,*line,rows,n),f32),
            V(3,rows,n),V(3,rows,n),DMA((2,12)),DMA((2,12))]
    COUNT=19
    def __init__(self,torus,order,out,halves,refs):
        self.t,self.order,self.out,self.halves=torus,order,out,halves
        (self.own,self.ds,self.dr,self.a1s,self.a1A,self.a1B,self.a2s,self.a2r,self.t1,
            self.b1s,self.b1A,self.b1B,self.b2s,self.b2r,self.t2,self.cs,self.cr,*self.sems)=refs
    @staticmethod
    def slot(ref,i):
        return lax.rem(i,ref.shape[0])
    def copies(self,stage,i):
        t=self.t
        first,b,a=self.order
        s=lax.rem(i,2)
        copy=lambda k,src,dst,to: remote(src,dst,self.sems,s,k,to)
        if stage==0: return [copy(0,self.ds.at[self.slot(self.ds,i)],self.dr.at[s],t.partner)]
        if stage==5: return [copy(9+d,self.cs.at[s,d],self.cr.at[s,d],to) for d,to in enumerate(t.ringid[first])]
        axis,k=(a,1) if stage<3 else (b,5)
        if stage%2:
            src,A,B=(self.a1s,self.a1A,self.a1B) if stage<3 else (self.b1s,self.b1A,self.b1B)
            lead=(ALL,)*(len(A.shape)-3)
            pieces=[(src.at[(s,*lead,*h)],dst.at[s]) for h,dst in zip(self.halves,(A,B),strict=True)]
        else:
            src,dst=(self.a2s,self.a2r) if stage<3 else (self.b2s,self.b2r)
            pieces=[(src.at[s,d],dst.at[s,d]) for d in range(2)]
            k+=2
        return [copy(k+d,*piece,to) for d,(piece,to) in enumerate(zip(pieces,(t.pid[axis],t.qid[axis]),strict=True))]
    def run(self,stage,i,column):
        t=self.t
        first,b,a=self.order
        s,o=lax.rem(i,2),self.slot(self.own,i)
        if stage>0:
            for cp in self.copies(stage-1,i): cp.wait()
        rem=[k for k in range(3) if k!=a]
        plane=lambda v: self.own[(o,*at(a,v))]
        line=lambda v: self.t1[(s,*at(b,v,rem))]
        axis,get=(a,plane) if stage<3 else (b,line)
        if stage==1:
            self.own[o]+=self.dr[s].astype(f32)
            self.a1s[s]=plane(t.ring[a][1]).astype(bf)
        elif stage==3:
            self.t1[s]=plane(t.xyz[a])+self.a2r[s,0].astype(f32)+self.a2r[s,1].astype(f32)
            self.b1s[s]=line(t.ring[b][1]).astype(bf)
        elif stage in (2,4):
            dst,came=(self.a2s,(self.a1A,self.a1B)) if stage==2 else (self.b2s,(self.b1A,self.b1B))
            for d,to in enumerate((t.p[axis],t.q[axis])):
                v=get(to)
                lead=(ALL,)*(v.ndim-2)
                for e,(r,c) in enumerate(self.halves):
                    part=v[(*lead,slice(r.start,r.start+r.size),slice(c.start,c.start+c.size))]
                    if d==e: part=part+came[e][s].astype(f32)
                    dst[(s,d,*lead,r,c)]=part.astype(bf)
        elif stage==5:
            self.t2[s]=line(t.xyz[b])+self.b2r[s,0].astype(f32)+self.b2r[s,1].astype(f32)
            for d,to in enumerate(t.ring[first]):
                self.cs[s,d]=self.t2[s,to].astype(bf)
        elif stage==6:
            v=self.t2[s,t.xyz[first]]
            for d in range(3): v=v+self.cr[s,d].astype(f32)
            self.out(column,v.astype(bf))
        if stage<6:
            for cp in self.copies(stage,i): cp.start()

def split(core,v0,v1):
    return jnp.where(core==0,v0,v1),jnp.where(core==0,v1,v0)

def b_kernel(x,dy,h1,ga,gb,pt,at_,wc,gg,gu,dx,og,ou,od,dgo,duo,
        odp,dhv,atv,both,abv,gsv,wdv,tiles,hv,dhsem,atsem,bothsem,absem,gssem,wdsem,tilesem,hsem,dxsem,*scr):
    torus=Torus()
    layer_of=lambda half: L-1-half
    def prefetch(half,j):
        l,s=layer_of(half),lax.rem(j,2)
        return [pltpu.make_async_copy(o.at[l,j],abv.at[m,s],absem.at[m,s]) for m,o in enumerate((ga,gb))]+[
            pltpu.make_async_copy(wc.at[l,aligned(j,COLS)],wdv.at[s],wdsem.at[s])]
    def load_at(half):
        return pltpu.make_async_copy(at_.at[layer_of(half)],atv,atsem)
    def load_pt(half):
        return [pltpu.make_async_copy(pt.at[aligned(layer_of(half),TILES*F)],both,bothsem.at[0])]
    def load_w(half):
        return [pltpu.make_async_copy(g.at[aligned(layer_of(half),NG*D)],both.at[pl.ds(m*NG*D,NG*D)],bothsem.at[m]) for m,g in enumerate((gg,gu))]
    def store_gs(j):
        s=lax.rem(j,2)
        return [pltpu.make_async_copy(gsv.at[m,s],o.at[j],gssem.at[m,s]) for m,o in enumerate((dgo,duo))]
    def load_tile(r):
        s=lax.rem(r,2)
        return [pltpu.make_async_copy(o.at[:,aligned(r,BM)],tiles.at[m,s],tilesem.at[m,s]) for m,o in enumerate((dgo,duo))]
    def load_h(half,r,go):
        s=lax.rem(r,2)
        for k,h in enumerate((h1,x)):
            @pl.when(half==k)
            def _():
                cp=pltpu.make_async_copy(h.at[aligned(r,BM)],hv.at[s],hsem.at[s])
                cp.start() if go else cp.wait()
    def store_dx(r):
        return pltpu.make_async_copy(dhv.at[aligned(r,BM)],dx.at[aligned(r,BM)],dxsem.at[r])
    def each(copies,go):
        for cp in copies: cp.start() if go else cp.wait()

    load_dh=pltpu.make_async_copy(dy,dhv,dhsem)
    load_dh.start()
    each(prefetch(0,0),True)
    load_at(0).start()
    torus.barrier()
    n=Scatter.COUNT
    def outs(half):
        l=layer_of(half)
        def gate(j,v): og[l,:,aligned(j,COLS)]=v
        def up(j,v): ou[l,:,aligned(j,COLS)]=v
        def down(k,v): odp[l,:,aligned(k,LANES)]=v
        return gate,up,down
    def scatters(half):
        return [Scatter(torus,order,out,h,scr[m*n:(m+1)*n]) for m,(order,out,h) in
            enumerate(zip(ORDERS,outs(half),(HALF_COLS,HALF_COLS,HALF_ROWS),strict=True))]
    eg,eu,ed=scatters(0)

    def tick(half,s):
        eg,eu,ed=scatters(half)
        for stage in reversed(range(S_STAGES)):
            j=s-SEND-stage
            @pl.when((j>=0)&(j<NG))
            def _():
                for e in (eg,eu): e.run(stage,half*NG+j,j)
                @pl.when((j>=DOWN)&(j<DOWN+ND))
                def _(): ed.run(stage,half*ND+j-DOWN,j-DOWN)

    def front(j):
        s=lax.rem(j,2)
        for r in range(TILES):
            rows=pl.ds(r*BM,BM)
            dp=dot(dhv[rows,:],wdv[s],1,1).astype(bf).astype(f32)
            for m in range(2):
                gsv[m,s,rows,:]=(dp*abv[m,s,rows,:]).astype(bf)
    def back(half,j):
        s,i=lax.rem(j,2),half*NG+j
        o,to=Scatter.slot(eg.own,i),Scatter.slot(eg.ds,i)
        for m,e in enumerate((eg,eu)):
            grad=gsv[m,s]
            for k in range(RING):
                v=dot(atv[pl.ds(k*BM,BM),:],grad).reshape(RING*RING,2,R8,COLS)
                own,other=split(torus.c,v[:,0],v[:,1])
                e.own[o,k]=own.reshape(RING,RING,R8,COLS)
                e.ds[to,k]=other.astype(bf).reshape(RING,RING,R8,COLS)
    def grad_down(half,k):
        dh=dhv[:,aligned(lax.div(k,2),COLS)]
        first=half*ND+k
        for g in range(RING*RING):
            rows=jnp.concatenate([both[pl.ds(r*F+g*GROUP,GROUP),:] for r in range(TILES)],1)
            v=dot(rows,dh)
            for z in range(RING):
                pair=[v[ROWS*d:ROWS*d+ROWS] for d in (2*z,2*z+1)]
                own,other=split(torus.c,*pair)
                other=other.astype(bf)
                for e in range(2):
                    cols=slice(e*LANES,e*LANES+LANES)
                    ed.own[Scatter.slot(ed.own,first+e),g//RING,g%RING,z,0:ROWS,:]=own[:,cols]
                    ed.ds[Scatter.slot(ed.ds,first+e),g//RING,g%RING,z,0:ROWS,:]=other[:,cols]
    def grad_h(half,r):
        s=lax.rem(r,2)
        acc=None
        for j in range(NG):
            for m in range(2):
                v=dot(tiles[m,s,j],both[pl.ds((m*NG+j)*D,D),:],1,1)
                acc=v if acc is None else acc+v
        d=acc.astype(bf).astype(f32)
        h=hv[s].astype(f32)
        scale=rms(h)
        through=jnp.sum(d*h,-1,keepdims=True)*(scale*scale*scale)*(1/D)
        rows=aligned(r,BM)
        dhv[rows,:]=dhv[rows,:]+(d*scale-h*through).astype(bf)
        @pl.when(half==L-1)
        def _(): store_dx(r).start()

    load_dh.wait()
    def step(now,carry):
        half,s=lax.div(now,B_STEPS),lax.rem(now,B_STEPS)
        r=s-B_TAIL
        tick(half,s)
        @pl.when(s==0)
        def _(): each(load_pt(half),True)
        @pl.when(s<NG-1)
        def _(): each(prefetch(half,s+1),True)
        @pl.when(s==DOWN+ND)
        def _(): each(load_w(half),True)
        @pl.when(s==B_TAIL-1)
        def _():
            each(store_gs(NG-1),False)
            each(store_gs(NG-2),False)
            each(load_tile(0),True)
            load_h(half,0,True)
        @pl.when(s==B_TAIL)
        def _(): each(load_w(half),False)
        @pl.when((s==B_TAIL)&(half<L-1))
        def _(): load_at(half+1).start()
        @pl.when((s>=B_TAIL)&(s<B_STEPS-1))
        def _():
            each(load_tile(r+1),True)
            load_h(half,r+1,True)
        @pl.when((s==B_STEPS-1)&(half<L-1))
        def _(): each(prefetch(half+1,0),True)
        @pl.when(s<NG)
        def _():
            each(prefetch(half,s),False)
            @pl.when(s>=2)
            def _(): each(store_gs(s-2),False)
        @pl.when(s==1)
        def _(): load_at(half).wait()
        @pl.when(s==DOWN)
        def _(): each(load_pt(half),False)
        @pl.when(s>=B_TAIL)
        def _():
            each(load_tile(r),False)
            load_h(half,r,False)
        @pl.when((s>=DOWN)&(s<DOWN+ND)&(lax.rem(s,2)==0))
        def _(): grad_down(half,s-DOWN)
        @pl.when(s==0)
        def _(): front(s)
        @pl.when((s>0)&(s<NG))
        def _():
            front(s); back(half,s-1)
        @pl.when(s==NG)
        def _(): back(half,s-1)
        @pl.when(s<NG)
        def _(): each(store_gs(s),True)
        @pl.when(s>=B_TAIL)
        def _(): grad_h(half,r)
        return carry
    lax.fori_loop(0,L*B_STEPS,step,0)
    for r in range(TILES): store_dx(r).wait()
    od[...]=odp[:,0:ROWS,:]

def backward(x,dy,h1,ga,gb,pt,at_,wc,gg,gu):
    return pl.pallas_call(b_kernel,
        out_shape=[S((M,D),bf),S((L,R8,F),bf),S((L,R8,F),bf),S((L,ROWS,D),bf)]+[S((NG,M,COLS),bf)]*2,
        in_specs=[ANY]*10,out_specs=[ANY]+[INVMEM]*3+[ANY]*2,
        scratch_shapes=[VMEM((L,PAD,D),bf),VMEM((M,D),bf),VMEM((D,M),bf),VMEM((TILES*F,COLS),bf),VMEM((2,2,M,COLS),f32),VMEM((2,2,M,COLS),bf),
            VMEM((2,COLS,D),bf),VMEM((2,2,NG,BM,COLS),bf),VMEM((2,BM,D),bf),
            DMA,DMA,DMA((2,)),DMA((2,2)),DMA((2,2)),DMA((2,)),DMA((2,2)),DMA((2,)),DMA((TILES,))]
            +Scatter.scratch(R8,COLS,HALF_COLS)*2+Scatter.scratch(PAD,LANES,HALF_ROWS,6,4),
        compiler_params=params(1,63),name="backward")(x,dy,h1,ga,gb,pt,at_,wc,gg,gu)

def step(x,dy,wg,wu,wd):
    x,dy=x[0],dy[0]
    gg,gu,_,ga,gb,pt,at_,h1,wc=forward(x,wg,wu,wd)
    gg,gu=(t.reshape(ITEMS*D,COLS) for t in (gg,gu))
    dx,og,ou,od,_,_=backward(x,dy,h1,ga,gb,pt.reshape(L*TILES*F,COLS),at_,wc,gg,gu)
    return dx[None],og,ou,od

def solution(mesh):
    tok=P(("rep","dp"),None,None)
    w=P(None,"dp",None)
    o=P("rep","dp",None)
    return jax.shard_map(step,mesh=mesh,in_specs=(tok,tok,w,w,w),out_specs=(tok,o,o,o),check_vma=False)
```

```python
import functools

import jax
import jax.numpy as jnp
from jax import lax
from jax.experimental import pallas as pl
from jax.experimental.pallas import tpu as pltpu
from jax.sharding import PartitionSpec as P

MESH=pl.DeviceIdType.MESH
bf=jnp.bfloat16
f32=jnp.float32
S=jax.ShapeDtypeStruct
ALLOF=...
ALL=slice(None)
M,D,F,L=2048,1024,2816,2
RING,COLS,LANES=4,256,128
CHIPS=(RING,)*3
TORUS=(*CHIPS,2)
R8,ROWS,PAD,EIGHT=8,22,24,8
GROUP=EIGHT*ROWS
NG,ND=F//COLS,D//LANES
ITEMS=L*NG
BM=256
TILES=M//BM
ORDERS=((2,1,0),(0,2,1),(1,0,2))
HALF_COLS=((pl.ds(0,R8),pl.ds(0,LANES)),(pl.ds(0,R8),pl.ds(LANES,LANES)))
HALF_ROWS=((pl.ds(0,16),pl.ds(0,LANES)),(pl.ds(16,8),pl.ds(0,LANES)))
DMA=pltpu.SemaphoreType.DMA
ANY=pl.BlockSpec(memory_space=pl.ANY)
INVMEM=pl.BlockSpec(memory_space=pltpu.VMEM)
VMEM=pltpu.VMEM

def dot(a,b,ca=1,cb=0):
    return lax.dot_general(a,b,(((ca,),(cb,)),((),())),preferred_element_type=f32)

def rms(h):
    return lax.rsqrt(jnp.mean(h*h,-1,keepdims=True)+1e-6)

def normed(h):
    wide=h.astype(f32)
    return (wide*rms(wide)).astype(bf)

def aligned(i,n):
    return pl.ds(pl.multiple_of(i*n,n),n)

def params(n,mb):
    return pltpu.CompilerParams(collective_id=n,has_side_effects=True,vmem_limit_bytes=mb<<20)


class Torus:
    def __init__(self):
        me=lax.axis_index("dp")
        chip,self.c=lax.div(me,2),lax.rem(me,2)
        self.xyz=(lax.div(chip,RING*RING),lax.rem(lax.div(chip,RING),RING),lax.rem(chip,RING))
        self.partner=me+1-2*self.c
        weight=(2*RING*RING,2*RING,2)
        sigma=1-2*self.c
        self.ring,self.ringid,self.p,self.q,self.pid,self.qid=[],[],[],[],[],[]
        for v,w in zip(self.xyz,weight,strict=True):
            place=lambda d: lax.rem(v+d,RING)
            ident=lambda u: me+(u-v)*w
            ring=[place(d) for d in range(1,RING)]
            p,q=place(RING+sigma),place(RING-sigma)
            for to,value in ((self.ring,ring),(self.ringid,[ident(u) for u in ring]),(self.p,p),(self.q,q),(self.pid,ident(p)),(self.qid,ident(q))):
                to.append(value)

    def barrier(self):
        b=pltpu.get_barrier_semaphore()
        reach=[to for ids in self.ringid for to in ids]+[self.partner]
        for to in reach:
            pl.semaphore_signal(b,inc=1,device_id={"dp":to},device_id_type=MESH)
        pl.semaphore_wait(b,len(reach))

def at(axis,v,axes=(0,1,2)):
    return tuple(v if k==axis else ALL for k in axes)

def remote(src,dst,sems,slot,k,to):
    send,recv=sems
    return pltpu.make_async_remote_copy(src_ref=src,dst_ref=dst,send_sem=send.at[slot,k],recv_sem=recv.at[slot,k],
        device_id={"dp":to},device_id_type=MESH)


SLOTS=4
G_OFF=(0,2,4,6,8,9)
G_LAST=len(G_OFF)-1
G_DEPTH=G_OFF[-1]
DM=TILES//2*BM
DOWN_STEPS=M//DM
F_STEPS=ITEMS+DOWN_STEPS

class Gather:
    COPIES=11
    def __init__(self,torus,order,g,own,shards,halves,sems,local):
        self.t,self.order,self.g,self.own,self.shards,self.halves,self.sems,self.local=torus,order,g,own,shards,halves,sems,local
    def region(self,i,full,axis=None,v=None,part=(ALL,ALL)):
        where=(ALL if k in full else v if k==axis else self.t.xyz[k] for k in range(3))
        return self.g.at[(i,*where,self.t.c,*part)]
    def pieces(self,stage,i):
        t=self.t
        a,b,last=self.order
        if stage==0:
            mine=self.region(i,())
            return [(self.own(i),mine,to) for to in t.ringid[a]]
        if stage==1:
            mine=self.region(i,(a,))
            return [(mine,mine,to) for to in t.ringid[b]]
        if stage==4:
            mine=self.region(i,(0,1,2))
            return [(mine,mine,t.partner)]
        to=(t.pid[last],t.qid[last])
        if stage==2:
            mine=self.region(i,(a,b))
            return [(mine,mine,to[d]) for d in range(2)]
        came=(t.q[last],t.p[last])
        parts=[self.region(i,(a,b),last,came[d],self.halves[d]) for d in range(2)]
        return [(parts[d],parts[d],to[d]) for d in range(2)]
    def copies(self,stage,i,slot):
        first=(0,3,6,8,10)[stage]
        send,recv=self.sems
        return [pltpu.make_async_remote_copy(src_ref=src,dst_ref=dst,send_sem=send.at[first+k],recv_sem=recv.at[slot,first+k],
            device_id={"dp":to},device_id_type=MESH) for k,(src,dst,to) in enumerate(self.pieces(stage,i))]
    def own_copy(self,i,slot):
        return pltpu.make_async_copy(self.own(i),self.region(i,()),self.local.at[slot])
    def run(self,stage,i):
        slot=lax.rem(i,SLOTS)
        if stage>0:
            for cp in self.copies(stage-1,i,slot): cp.wait_recv()
            if stage==1: self.own_copy(i,slot).wait()
        if stage<G_LAST:
            for cp in self.copies(stage,i,slot): cp.start()
            if stage==0: self.own_copy(i,slot).start()
    def drain(self):
        self.own=lambda i: self.shards
        for stage in range(G_LAST):
            for k,cp in enumerate(self.copies(stage,ALL,0)): cp.wait_send()

def f_kernel(x,wg,wu,wd,gg,gu,gd,ga,gb,pt,at_,h1,wc,
        wdp,xv,av,ptv,wcv,wv,dv,abv,atv,hv,xsem,wsem,dsem,absem,ptsem,atsem,hsem,wcsem,*gsems):
    for l in range(L):
        wdp[l,0:ROWS,:]=wd[:,l,:]
        wdp[l,ROWS:PAD,:]=jnp.zeros((PAD-ROWS,D),bf)
    load_x=pltpu.make_async_copy(x,xv,xsem)
    load_x.start()
    torus=Torus()
    torus.barrier()
    own_g=lambda i: wg.at[lax.div(i,NG),:,aligned(lax.rem(i,NG),COLS)]
    own_u=lambda i: wu.at[lax.div(i,NG),:,aligned(lax.rem(i,NG),COLS)]
    own_d=lambda k: wdp.at[lax.div(k,ND),:,aligned(lax.rem(k,ND),LANES)]
    eg=Gather(torus,ORDERS[0],gg,own_g,wg,HALF_COLS,gsems[0:2],gsems[2])
    eu=Gather(torus,ORDERS[1],gu,own_u,wu,HALF_COLS,gsems[3:5],gsems[5])
    ed=Gather(torus,ORDERS[2],gd,own_d,wdp,HALF_ROWS,gsems[6:8],gsems[8])
    def load_d(k):
        return pltpu.make_async_copy(gd.at[k],dv.at[lax.rem(k,2)],dsem.at[lax.rem(k,2)])
    def store_wc(l):
        return pltpu.make_async_copy(wcv.at[l],wc.at[l],wcsem.at[l])
    def compact(k):
        load_d(k).wait()
        def plane(x,carry):
            for y in range(RING):
                v=dv[lax.rem(k,2),x,y].reshape(EIGHT,PAD,LANES).astype(f32)
                wcv[lax.div(k,ND),aligned(x*RING+y,GROUP),aligned(lax.rem(k,ND),LANES)]=jnp.concatenate([v[d,0:ROWS] for d in range(EIGHT)],0).astype(bf)
            return carry
        lax.fori_loop(0,RING,plane,0)
        @pl.when(lax.rem(k,ND)==ND-1)
        def _(): store_wc(lax.div(k,ND)).start()
    def tick(t):
        i=t-G_DEPTH-1
        @pl.when((i>=0)&(i<L*ND))
        def _(): compact(i)
        for stage in reversed(range(G_LAST+1)):
            i=t-G_OFF[stage]
            @pl.when((i>=0)&(i<ITEMS))
            def _():
                eg.run(stage,i); eu.run(stage,i)
                @pl.when(i<L*ND)
                def _():
                    ed.run(stage,i)
                    if stage==G_LAST: load_d(i).start()
    item_of=lambda k: jnp.where(k<NG,k,k-DOWN_STEPS)
    is_item=lambda k: ((k>=0)&(k<NG))|((k>=NG+DOWN_STEPS)&(k<F_STEPS))
    def load_w(i):
        return [pltpu.make_async_copy(g.at[i],wv.at[m,lax.rem(i,2)],wsem.at[m,lax.rem(i,2)]) for m,g in enumerate((gg,gu))]
    def store_ab(i):
        s=lax.rem(i,2)
        return [pltpu.make_async_copy(abv.at[m,s],o.at[lax.div(i,NG),lax.rem(i,NG)],absem.at[m,s]) for m,o in enumerate((ga,gb))]+[
            pltpu.make_async_copy(ptv.at[:,aligned(lax.rem(i,NG),COLS)],pt.at[lax.div(i,NG),:,aligned(lax.rem(i,NG),COLS)],ptsem.at[s])]
    def store_at(l,r):
        return pltpu.make_async_copy(atv.at[r],at_.at[l,:,aligned(r,DM)],atsem.at[r])
    def store_h(r):
        return pltpu.make_async_copy(hv.at[r],h1.at[aligned(r,DM)],hsem.at[r])
    def put_a(slot,tile,first,h):
        a=normed(h)
        av[pl.ds(first,BM),:]=a
        atv[slot,:,pl.ds(tile*BM,BM)]=a.T
    def gate_up(i):
        for cp in load_w(i): cp.wait()
        @pl.when(i>=2)
        def _():
            for cp in store_ab(i-2): cp.wait()
        s=lax.rem(i,2)
        w_gate,w_up=(wv[m,s].reshape(D,COLS) for m in range(2))
        for r in range(TILES):
            rows=pl.ds(r*BM,BM)
            g=dot(av[rows,:],w_gate)
            u=dot(av[rows,:],w_up)
            sg=jax.nn.sigmoid(g)
            b=g*sg
            abv[0,s,rows,:]=u*(sg+b*(1-sg))
            abv[1,s,rows,:]=b
            ptv[r,aligned(lax.rem(i,NG),COLS),:]=(b*u).astype(bf).T
        for cp in store_ab(i): cp.start()
    def down(r):
        store_at(0,r).wait()
        for tile in range(DM//BM):
            first=pl.multiple_of(r*DM+tile*BM,BM)
            y=dot(ptv[r*(DM//BM)+tile],wcv[0],0,0).astype(bf)
            h=xv[pl.ds(first,BM),:]+y
            hv[r,pl.ds(tile*BM,BM),:]=h
            put_a(r,tile,first,h)
        store_h(r).start()
        store_at(1,r).start()
    tick(0)
    load_x.wait()
    for r in range(DOWN_STEPS):
        def norm(tile,carry):
            first=pl.multiple_of(r*DM+tile*BM,BM)
            a=normed(xv[pl.ds(first,BM),:])
            av[pl.ds(first,BM),:]=a
            atv[r,:,aligned(tile,BM)]=a.T
            return carry
        lax.fori_loop(0,DM//BM,norm,0)
        store_at(0,r).start()
    def step(t,carry):
        k=t-G_DEPTH-1
        tick(t)
        @pl.when(is_item(k+1))
        def _():
            for cp in load_w(item_of(k+1)): cp.start()
        @pl.when(is_item(k))
        def _(): gate_up(item_of(k))
        @pl.when((k>=NG)&(k<NG+DOWN_STEPS))
        def _(): down(k-NG)
        return carry
    lax.fori_loop(1,F_STEPS+G_DEPTH+1,step,0)
    for r in range(DOWN_STEPS):
        store_at(1,r).wait()
        store_h(r).wait()
    for e in (eg,eu,ed): e.drain()
    for i in (ITEMS-2,ITEMS-1):
        for cp in store_ab(i): cp.wait()
    for l in range(L): store_wc(l).wait()

def forward(x,wg,wu,wd):
    return pl.pallas_call(f_kernel,
        out_shape=[S((ITEMS,*TORUS,R8,COLS),bf)]*2+[S((L*ND,*TORUS,PAD,LANES),bf)]+[S((L,NG,M,COLS),f32)]*2+[
            S((L,TILES,F,BM),bf),S((L,D,M),bf),S((M,D),bf),S((L,F,D),bf)],
        in_specs=[ANY]+[INVMEM]*3,out_specs=[ANY]*9,
        scratch_shapes=[VMEM((L,PAD,D),bf),VMEM((M,D),bf),VMEM((M,D),bf),VMEM((TILES,F,BM),bf),VMEM((L,F,D),bf),VMEM((2,2,*TORUS,R8,COLS),bf),
            VMEM((2,*TORUS,PAD,LANES),bf),VMEM((2,2,M,COLS),f32),VMEM((DOWN_STEPS,D,DM),bf),VMEM((DOWN_STEPS,DM,D),bf),
            DMA,DMA((2,2)),DMA((2,)),DMA((2,2)),DMA((2,)),DMA((DOWN_STEPS,)),DMA((DOWN_STEPS,)),DMA((L,))]+[DMA((Gather.COPIES,)),DMA((SLOTS,Gather.COPIES)),DMA((SLOTS,))]*3,
        compiler_params=params(0,62),name="forward")(x,wg,wu,wd)


B_TAIL=NG+1
B_STEPS=B_TAIL+TILES
SEND,DOWN=2,2
S_STAGES=6

class Scatter:
    @staticmethod
    def scratch(rows,n,halves,own=4,ds=2):
        V=lambda *s: VMEM((2,*s),bf)
        A,B=((r.size,c.size) for r,c in halves)
        plane,line=(RING,RING),(RING,)
        return [VMEM((own,*CHIPS,rows,n),f32),VMEM((ds,*CHIPS,rows,n),bf),VMEM((4,*CHIPS,rows,n),bf),
            V(*plane,rows,n),V(*plane,*A),V(*plane,*B),V(2,*plane,rows,n),V(2,*plane,rows,n),VMEM((2,*plane,rows,n),f32),
            V(3,*line,rows,n),V(3,*line,rows,n),VMEM((2,*line,rows,n),f32),V(3,rows,n),V(3,rows,n),DMA((2,Scatter.COPIES)),DMA((2,Scatter.COPIES))]
    COUNT,COPIES=16,11
    def __init__(self,torus,order,out,halves,refs):
        self.t,self.order,self.out,self.halves=torus,order,out,halves
        self.own,self.ds,self.dr,self.a1s,self.a1A,self.a1B,self.a2s,self.a2r,self.t1,self.bs,self.br,self.t2,self.cs,self.cr,*self.sems=refs
    @staticmethod
    def slot(ref,i):
        return lax.rem(i,ref.shape[0])
    def copies(self,stage,i):
        t=self.t
        first,b,a=self.order
        s=lax.rem(i,2)
        k=(0,1,3,5,8)[stage]
        to=(t.pid[a],t.qid[a])
        if stage==0: pieces=[(self.ds.at[self.slot(self.ds,i)],self.dr.at[self.slot(self.dr,i)],t.partner)]
        elif stage==1: pieces=[(self.a1s.at[(s,ALL,ALL,*h)],dst.at[s],to[d]) for d,(h,dst) in enumerate(zip(self.halves,(self.a1A,self.a1B),strict=True))]
        elif stage==2: pieces=[(self.a2s.at[s,d],self.a2r.at[s,d],to[d]) for d in range(2)]
        else:
            src,dst,ids=(self.bs,self.br,t.ringid[b]) if stage==3 else (self.cs,self.cr,t.ringid[first])
            pieces=[(src.at[s,d],dst.at[s,d],ids[d]) for d in range(3)]
        return [remote(src,dst,self.sems,s,k+d,dev) for d,(src,dst,dev) in enumerate(pieces)]
    def run(self,stage,i,column):
        t=self.t
        first,b,a=self.order
        s,o,r=lax.rem(i,2),self.slot(self.own,i),self.slot(self.dr,i)
        if stage>0:
            for cp in self.copies(stage-1,i): cp.wait()
        rem=[k for k in range(3) if k!=a]
        plane=lambda v: self.own[(o,*at(a,v))]+self.dr[(r,*at(a,v))].astype(f32)
        line=lambda v: self.t1[(s,*at(b,v,rem))]
        came=lambda ref: (ref[s,d].astype(f32) for d in range(ref.shape[1]))
        if stage==1:
            self.a1s[s]=plane(t.ring[a][1]).astype(bf)
        elif stage==2:
            for d,to in enumerate((t.p[a],t.q[a])):
                v=plane(to)
                for e,(rows,cols) in enumerate(self.halves):
                    part=v[:,:,rows.start:rows.start+rows.size,cols.start:cols.start+cols.size]
                    if d==e: part=part+(self.a1A,self.a1B)[e][s].astype(f32)
                    self.a2s[s,d,:,:,rows,cols]=part.astype(bf)
        elif stage==3:
            self.t1[s]=sum(came(self.a2r),plane(t.xyz[a]))
            for d,to in enumerate(t.ring[b]): self.bs[s,d]=line(to).astype(bf)
        elif stage==4:
            self.t2[s]=sum(came(self.br),line(t.xyz[b]))
            for d,to in enumerate(t.ring[first]): self.cs[s,d]=self.t2[s,to].astype(bf)
        elif stage==5:
            self.out(column,sum(came(self.cr),self.t2[s,t.xyz[first]]).astype(bf))
        if stage<5:
            for cp in self.copies(stage,i): cp.start()

def split(core,v0,v1):
    return jnp.where(core==0,v0,v1),jnp.where(core==0,v1,v0)

def b_kernel(x,dy,h1,ga,gb,pt,at_,wc,gg,gu,dx,og,ou,od,dgo,duo,
        odp,dhv,atv,both,abv,gsv,wdv,tiles,hv,dhsem,atsem,bothsem,absem,gssem,wdsem,tilesem,hsem,dxsem,*scr):
    torus=Torus()
    layer_of=lambda half: L-1-half
    def prefetch(half,j):
        l,s=layer_of(half),lax.rem(j,2)
        return [pltpu.make_async_copy(o.at[l,j],abv.at[m,s],absem.at[m,s]) for m,o in enumerate((ga,gb))]+[
            pltpu.make_async_copy(wc.at[l,aligned(j,COLS)],wdv.at[s],wdsem.at[s])]
    def load_at(half):
        return pltpu.make_async_copy(at_.at[layer_of(half)],atv,atsem)
    def load_pt(half):
        return [pltpu.make_async_copy(pt.at[aligned(layer_of(half),TILES*F)],both,bothsem.at[0])]
    def load_w(half):
        return [pltpu.make_async_copy(g.at[aligned(layer_of(half),NG*D)],both.at[pl.ds(m*NG*D,NG*D)],bothsem.at[m]) for m,g in enumerate((gg,gu))]
    def store_gs(j):
        s=lax.rem(j,2)
        return [pltpu.make_async_copy(gsv.at[m,s],o.at[j],gssem.at[m,s]) for m,o in enumerate((dgo,duo))]
    def load_tile(r):
        s=lax.rem(r,2)
        return [pltpu.make_async_copy(o.at[:,aligned(r,BM)],tiles.at[m,s],tilesem.at[m,s]) for m,o in enumerate((dgo,duo))]
    def load_h(half,r,go):
        s=lax.rem(r,2)
        for k,h in enumerate((h1,x)):
            @pl.when(half==k)
            def _():
                cp=pltpu.make_async_copy(h.at[aligned(r,BM)],hv.at[s],hsem.at[s])
                cp.start() if go else cp.wait()
    def store_dx(r):
        return pltpu.make_async_copy(dhv.at[aligned(r,BM)],dx.at[aligned(r,BM)],dxsem.at[r])
    def each(copies,go):
        for cp in copies: cp.start() if go else cp.wait()

    load_dh=pltpu.make_async_copy(dy,dhv,dhsem)
    load_dh.start()
    each(prefetch(0,0),True)
    load_at(0).start()
    torus.barrier()
    n=Scatter.COUNT
    def outs(half):
        l=layer_of(half)
        def gate(j,v): og[l,:,aligned(j,COLS)]=v
        def up(j,v): ou[l,:,aligned(j,COLS)]=v
        def down(k,v): odp[l,:,aligned(k,LANES)]=v
        return gate,up,down
    def scatters(half):
        return [Scatter(torus,order,out,h,scr[m*n:(m+1)*n]) for m,(order,out,h) in
            enumerate(zip(ORDERS,outs(half),(HALF_COLS,HALF_COLS,HALF_ROWS),strict=True))]
    eg,eu,ed=scatters(0)

    def tick(half,s):
        eg,eu,ed=scatters(half)
        for stage in reversed(range(S_STAGES)):
            j=s-SEND-stage
            @pl.when((j>=0)&(j<NG))
            def _():
                for e in (eg,eu): e.run(stage,half*NG+j,j)
                @pl.when((j>=DOWN)&(j<DOWN+ND))
                def _(): ed.run(stage,half*ND+j-DOWN,j-DOWN)

    def front(j):
        s=lax.rem(j,2)
        for r in range(TILES):
            rows=pl.ds(r*BM,BM)
            dp=dot(dhv[rows,:],wdv[s],1,1).astype(bf).astype(f32)
            for m in range(2):
                gsv[m,s,rows,:]=(dp*abv[m,s,rows,:]).astype(bf)
    def back(half,j):
        s,i=lax.rem(j,2),half*NG+j
        o,to=Scatter.slot(eg.own,i),Scatter.slot(eg.ds,i)
        for m,e in enumerate((eg,eu)):
            grad=gsv[m,s]
            for k in range(RING):
                v=dot(atv[pl.ds(k*BM,BM),:],grad).reshape(RING*RING,2,R8,COLS)
                own,other=split(torus.c,v[:,0],v[:,1])
                e.own[o,k]=own.reshape(RING,RING,R8,COLS)
                e.ds[to,k]=other.astype(bf).reshape(RING,RING,R8,COLS)
    def grad_down(half,k):
        dh=dhv[:,aligned(lax.div(k,2),COLS)]
        first=half*ND+k
        for g in range(RING*RING):
            rows=jnp.concatenate([both[pl.ds(r*F+g*GROUP,GROUP),:] for r in range(TILES)],1)
            v=dot(rows,dh)
            for z in range(RING):
                pair=[v[ROWS*d:ROWS*d+ROWS] for d in (2*z,2*z+1)]
                own,other=split(torus.c,*pair)
                other=other.astype(bf)
                for e in range(2):
                    cols=slice(e*LANES,e*LANES+LANES)
                    ed.own[Scatter.slot(ed.own,first+e),g//RING,g%RING,z,0:ROWS,:]=own[:,cols]
                    ed.ds[Scatter.slot(ed.ds,first+e),g//RING,g%RING,z,0:ROWS,:]=other[:,cols]
    def grad_h(half,r):
        s=lax.rem(r,2)
        acc=None
        for j in range(NG):
            for m in range(2):
                v=dot(tiles[m,s,j],both[pl.ds((m*NG+j)*D,D),:],1,1)
                acc=v if acc is None else acc+v
        d=acc.astype(bf).astype(f32)
        h=hv[s].astype(f32)
        scale=rms(h)
        through=jnp.sum(d*h,-1,keepdims=True)*(scale*scale*scale)*(1/D)
        rows=aligned(r,BM)
        dhv[rows,:]=dhv[rows,:]+(d*scale-h*through).astype(bf)
        @pl.when(half==L-1)
        def _(): store_dx(r).start()

    load_dh.wait()
    def step(now,carry):
        half,s=lax.div(now,B_STEPS),lax.rem(now,B_STEPS)
        r=s-B_TAIL
        tick(half,s)
        @pl.when(s==0)
        def _(): each(load_pt(half),True)
        @pl.when(s<NG-1)
        def _(): each(prefetch(half,s+1),True)
        @pl.when(s==DOWN+ND)
        def _(): each(load_w(half),True)
        @pl.when(s==B_TAIL-1)
        def _():
            each(store_gs(NG-1),False)
            each(store_gs(NG-2),False)
            each(load_tile(0),True)
            load_h(half,0,True)
        @pl.when(s==B_TAIL)
        def _(): each(load_w(half),False)
        @pl.when((s==B_TAIL)&(half<L-1))
        def _(): load_at(half+1).start()
        @pl.when((s>=B_TAIL)&(s<B_STEPS-1))
        def _():
            each(load_tile(r+1),True)
            load_h(half,r+1,True)
        @pl.when((s==B_STEPS-1)&(half<L-1))
        def _(): each(prefetch(half+1,0),True)
        @pl.when(s<NG)
        def _():
            each(prefetch(half,s),False)
            @pl.when(s>=2)
            def _(): each(store_gs(s-2),False)
        @pl.when(s==1)
        def _(): load_at(half).wait()
        @pl.when(s==DOWN)
        def _(): each(load_pt(half),False)
        @pl.when(s>=B_TAIL)
        def _():
            each(load_tile(r),False)
            load_h(half,r,False)
        @pl.when((s>=DOWN)&(s<DOWN+ND)&(lax.rem(s,2)==0))
        def _(): grad_down(half,s-DOWN)
        @pl.when(s==0)
        def _(): front(s)
        @pl.when((s>0)&(s<NG))
        def _():
            front(s); back(half,s-1)
        @pl.when(s==NG)
        def _(): back(half,s-1)
        @pl.when(s<NG)
        def _(): each(store_gs(s),True)
        @pl.when(s>=B_TAIL)
        def _(): grad_h(half,r)
        return carry
    lax.fori_loop(0,L*B_STEPS,step,0)
    for r in range(TILES): store_dx(r).wait()
    for l in range(L): od[:,l,:]=odp[l,0:ROWS,:]

def backward(x,dy,h1,ga,gb,pt,at_,wc,gg,gu):
    return pl.pallas_call(b_kernel,
        out_shape=[S((M,D),bf),S((L,R8,F),bf),S((L,R8,F),bf),S((ROWS,L,D),bf)]+[S((NG,M,COLS),bf)]*2,
        in_specs=[ANY]*10,out_specs=[ANY]+[INVMEM]*3+[ANY]*2,
        scratch_shapes=[VMEM((L,PAD,D),bf),VMEM((M,D),bf),VMEM((D,M),bf),VMEM((TILES*F,COLS),bf),VMEM((2,2,M,COLS),f32),VMEM((2,2,M,COLS),bf),
            VMEM((2,COLS,D),bf),VMEM((2,2,NG,BM,COLS),bf),VMEM((2,BM,D),bf),
            DMA,DMA,DMA((2,)),DMA((2,2)),DMA((2,2)),DMA((2,)),DMA((2,2)),DMA((2,)),DMA((TILES,))]
            +Scatter.scratch(R8,COLS,HALF_COLS)*2+Scatter.scratch(PAD,LANES,HALF_ROWS,6,4),
        compiler_params=params(1,63),name="backward")(x,dy,h1,ga,gb,pt,at_,wc,gg,gu)

def finish_kernel(*refs):
    n=len(refs)//4
    src,dst,held,sems=(refs[k*n:k*n+n] for k in range(4))
    def parts(r):
        size=r.shape[0]//4 if r.shape[0]==M else r.shape[0]
        return [pl.ds(k,size) for k in range(0,r.shape[0],size)]
    jobs=[(m,k,p) for m in range(n) for k,p in enumerate(parts(src[m]))]
    load=lambda m,k,p: pltpu.make_async_copy(src[m].at[p],held[m].at[p],sems[m].at[0,k])
    store=lambda m,k,p: pltpu.make_async_copy(held[m].at[p],dst[m].at[p],sems[m].at[1,k])
    for job in jobs: load(*job).start()
    for job in jobs:
        load(*job).wait()
        store(*job).start()
    for job in jobs: store(*job).wait()

def finish(*arrays):
    n=len(arrays)
    return pl.pallas_call(finish_kernel,out_shape=[S(t.shape,t.dtype) for t in arrays],in_specs=[ANY]*n,out_specs=[ANY]*n,
        scratch_shapes=[VMEM(t.shape,t.dtype) for t in arrays]+[DMA((2,4))]*n,
        compiler_params=pltpu.CompilerParams(vmem_limit_bytes=62<<20),name="finish")(*arrays)

def step(x,dy,wg,wu,wd):
    x,dy=x[0],dy[0]
    gg,gu,_,ga,gb,pt,at_,h1,wc=forward(x,wg,wu,jnp.swapaxes(wd,0,1))
    gg,gu=(t.reshape(ITEMS*D,COLS) for t in (gg,gu))
    dx,og,ou,od,_,_=backward(x,dy,h1,ga,gb,pt.reshape(L*TILES*F,COLS),at_,wc,gg,gu)
    dx,og,ou,od=finish(dx,og,ou,od)
    return dx[None],og,ou,jnp.swapaxes(od,0,1)

def solution(mesh):
    tok=P(("rep","dp"),None,None)
    w=P(None,"dp",None)
    o=P("rep","dp",None)
    return jax.shard_map(step,mesh=mesh,in_specs=(tok,tok,w,w,w),out_specs=(tok,o,o,o),check_vma=False)
```

```python
import functools

import jax
import jax.numpy as jnp
from jax import lax
from jax.experimental import pallas as pl
from jax.experimental.pallas import tpu as pltpu
from jax.sharding import PartitionSpec as P

MESH=pl.DeviceIdType.MESH
bf=jnp.bfloat16
f32=jnp.float32
S=jax.ShapeDtypeStruct
ALLOF=...
ALL=slice(None)
M,D,F,L=2048,1024,2816,2
RING,COLS,LANES=4,256,128
CHIPS=(RING,)*3
TORUS=(*CHIPS,2)
R8,ROWS,PAD,EIGHT=8,22,24,8
GROUP=EIGHT*ROWS
NG,ND=F//COLS,D//LANES
ITEMS=L*NG
BM=256
TILES=M//BM
ORDERS=((2,1,0),(2,0,1),(1,0,2))
HALF_COLS=((pl.ds(0,R8),pl.ds(0,LANES)),(pl.ds(0,R8),pl.ds(LANES,LANES)))
HALF_ROWS=((pl.ds(0,16),pl.ds(0,LANES)),(pl.ds(16,8),pl.ds(0,LANES)))
DMA=pltpu.SemaphoreType.DMA
ANY=pl.BlockSpec(memory_space=pl.ANY)
INVMEM=pl.BlockSpec(memory_space=pltpu.VMEM)
VMEM=pltpu.VMEM

def dot(a,b,ca=1,cb=0):
    return lax.dot_general(a,b,(((ca,),(cb,)),((),())),preferred_element_type=f32)

def rms(h):
    return lax.rsqrt(jnp.mean(h*h,-1,keepdims=True)+1e-6)

def normed(h):
    wide=h.astype(f32)
    return (wide*rms(wide)).astype(bf)

def aligned(i,n):
    return pl.ds(pl.multiple_of(i*n,n),n)

def params(n,mb):
    return pltpu.CompilerParams(collective_id=n,has_side_effects=True,vmem_limit_bytes=mb<<20)


class Torus:
    def __init__(self):
        me=lax.axis_index("dp")
        chip,self.c=lax.div(me,2),lax.rem(me,2)
        self.xyz=(lax.div(chip,RING*RING),lax.rem(lax.div(chip,RING),RING),lax.rem(chip,RING))
        self.partner=me+1-2*self.c
        weight=(2*RING*RING,2*RING,2)
        sigma=1-2*self.c
        self.ring,self.ringid,self.p,self.q,self.pid,self.qid=[],[],[],[],[],[]
        for v,w in zip(self.xyz,weight,strict=True):
            place=lambda d: lax.rem(v+d,RING)
            ident=lambda u: me+(u-v)*w
            ring=[place(d) for d in range(1,RING)]
            p,q=place(RING+sigma),place(RING-sigma)
            for to,value in ((self.ring,ring),(self.ringid,[ident(u) for u in ring]),(self.p,p),(self.q,q),(self.pid,ident(p)),(self.qid,ident(q))):
                to.append(value)

    def barrier(self):
        b=pltpu.get_barrier_semaphore()
        reach=[to for ids in self.ringid for to in ids]+[self.partner]
        for to in reach:
            pl.semaphore_signal(b,inc=1,device_id={"dp":to},device_id_type=MESH)
        pl.semaphore_wait(b,len(reach))

def at(axis,v,axes=(0,1,2)):
    return tuple(v if k==axis else ALL for k in axes)

def remote(src,dst,sems,slot,k,to):
    send,recv=sems
    return pltpu.make_async_remote_copy(src_ref=src,dst_ref=dst,send_sem=send.at[slot,k],recv_sem=recv.at[slot,k],
        device_id={"dp":to},device_id_type=MESH)


SLOTS=4
G_STAGES=("block","line","plane","pass plane","core","end")
D_STAGES=("block","near line","pass line","plane","pass plane","core","end")
COPIES={"block":3,"line":3,"near line":2,"pass line":2,"plane":2,"pass plane":2,"core":1,"end":0}
G_OFF=(0,2,4,6,8,9)
D_OFF=(0,2,4,6,8,10,11)
G_DEPTH=G_OFF[-1]
D_START=(2,2+ND+2)
DM=TILES//2*BM
DOWN_STEPS=M//DM
F_STEPS=ITEMS+DOWN_STEPS

class Gather:
    def __init__(self,torus,order,stages,g,own,shards,halves,sems,local):
        self.t,self.order,self.stages,self.g,self.own,self.shards,self.halves,self.sems,self.local=torus,order,stages,g,own,shards,halves,sems,local
    def region(self,i,full,axis=None,v=None,part=(ALL,ALL)):
        where=(ALL if k in full else v if k==axis else self.t.xyz[k] for k in range(3))
        return self.g.at[(i,*where,self.t.c,*part)]
    def pieces(self,stage,i):
        t=self.t
        a,b,last=self.order
        kind=self.stages[stage]
        if kind=="block":
            mine=self.region(i,())
            return [(self.own(i),mine,to) for to in t.ringid[a]]
        if kind=="core":
            mine=self.region(i,(0,1,2))
            return [(mine,mine,t.partner)]
        axis,full=(last,(a,b)) if kind.endswith("plane") else (b,(a,))
        to=t.ringid[axis] if kind=="line" else (t.pid[axis],t.qid[axis])
        if kind.startswith("pass"):
            came=(t.q[axis],t.p[axis])
            parts=[self.region(i,full,axis,came[d],self.halves[d]) for d in range(2)]
            return [(parts[d],parts[d],to[d]) for d in range(2)]
        mine=self.region(i,full)
        return [(mine,mine,dev) for dev in to]
    def copies(self,stage,i,slot):
        first=sum(COPIES[k] for k in self.stages[:stage])
        send,recv=self.sems
        return [pltpu.make_async_remote_copy(src_ref=src,dst_ref=dst,send_sem=send.at[first+k],recv_sem=recv.at[slot,first+k],
            device_id={"dp":to},device_id_type=MESH) for k,(src,dst,to) in enumerate(self.pieces(stage,i))]
    def own_copy(self,i,slot):
        return pltpu.make_async_copy(self.own(i),self.region(i,()),self.local.at[slot])
    def run(self,stage,i):
        slot=lax.rem(i,SLOTS)
        if stage>0:
            for cp in self.copies(stage-1,i,slot): cp.wait_recv()
            if stage==1: self.own_copy(i,slot).wait()
        if stage<len(self.stages)-1:
            for cp in self.copies(stage,i,slot): cp.start()
            if stage==0: self.own_copy(i,slot).start()
    def drain(self):
        self.own=lambda i: self.shards
        for stage in range(len(self.stages)-1):
            for cp in self.copies(stage,ALL,0): cp.wait_send()

def f_kernel(x,wg,wu,wd,gg,gu,gd,ga,gb,pt,at_,h1,wc,
        wdp,xv,av,ptv,wcv,wv,dv,abv,atv,hv,xsem,wsem,dsem,absem,ptsem,atsem,hsem,wcsem,*gsems):
    for l in range(L):
        wdp[l,0:ROWS,:]=wd[:,l,:]
        wdp[l,ROWS:PAD,:]=jnp.zeros((PAD-ROWS,D),bf)
    load_x=pltpu.make_async_copy(x,xv,xsem)
    load_x.start()
    torus=Torus()
    torus.barrier()
    own_g=lambda i: wg.at[lax.div(i,NG),:,aligned(lax.rem(i,NG),COLS)]
    own_u=lambda i: wu.at[lax.div(i,NG),:,aligned(lax.rem(i,NG),COLS)]
    own_d=lambda k: wdp.at[lax.div(k,ND),:,aligned(lax.rem(k,ND),LANES)]
    eg=Gather(torus,ORDERS[0],G_STAGES,gg,own_g,wg,HALF_COLS,gsems[0:2],gsems[2])
    eu=Gather(torus,ORDERS[1],G_STAGES,gu,own_u,wu,HALF_COLS,gsems[3:5],gsems[5])
    ed=Gather(torus,ORDERS[2],D_STAGES,gd,own_d,wdp,HALF_ROWS,gsems[6:8],gsems[8])
    def load_d(k):
        return pltpu.make_async_copy(gd.at[k],dv.at[lax.rem(k,2)],dsem.at[lax.rem(k,2)])
    def store_wc(l):
        return pltpu.make_async_copy(wcv.at[l],wc.at[l],wcsem.at[l])
    def compact(k):
        load_d(k).wait()
        def plane(x,carry):
            for y in range(RING):
                v=dv[lax.rem(k,2),x,y].reshape(EIGHT,PAD,LANES).astype(f32)
                wcv[lax.div(k,ND),aligned(x*RING+y,GROUP),aligned(lax.rem(k,ND),LANES)]=jnp.concatenate([v[d,0:ROWS] for d in range(EIGHT)],0).astype(bf)
            return carry
        lax.fori_loop(0,RING,plane,0)
        @pl.when(lax.rem(k,ND)==ND-1)
        def _(): store_wc(lax.div(k,ND)).start()
    def when_down(u,run):
        second=(u>=D_START[1])&(u<D_START[1]+ND)
        @pl.when(((u>=D_START[0])&(u<D_START[0]+ND))|second)
        def _(): run(u-jnp.where(u>=D_START[1],D_START[1]-ND,D_START[0]))
    def run_down(stage,k):
        ed.run(stage,k)
        if stage==len(D_STAGES)-1: load_d(k).start()
    def tick(t):
        when_down(t-D_OFF[-1]-1,compact)
        for stage in reversed(range(len(D_STAGES))):
            when_down(t-D_OFF[stage],functools.partial(run_down,stage))
        for stage in reversed(range(len(G_STAGES))):
            i=t-G_OFF[stage]
            @pl.when((i>=0)&(i<ITEMS))
            def _():
                eg.run(stage,i); eu.run(stage,i)
    item_of=lambda k: jnp.where(k<NG,k,k-DOWN_STEPS)
    is_item=lambda k: ((k>=0)&(k<NG))|((k>=NG+DOWN_STEPS)&(k<F_STEPS))
    def load_w(i):
        return [pltpu.make_async_copy(g.at[i],wv.at[m,lax.rem(i,2)],wsem.at[m,lax.rem(i,2)]) for m,g in enumerate((gg,gu))]
    def store_ab(i):
        s=lax.rem(i,2)
        return [pltpu.make_async_copy(abv.at[m,s],o.at[lax.div(i,NG),lax.rem(i,NG)],absem.at[m,s]) for m,o in enumerate((ga,gb))]+[
            pltpu.make_async_copy(ptv.at[:,aligned(lax.rem(i,NG),COLS)],pt.at[lax.div(i,NG),:,aligned(lax.rem(i,NG),COLS)],ptsem.at[s])]
    def store_at(l,r):
        return pltpu.make_async_copy(atv.at[r],at_.at[l,:,aligned(r,DM)],atsem.at[r])
    def store_h(r):
        return pltpu.make_async_copy(hv.at[r],h1.at[aligned(r,DM)],hsem.at[r])
    def put_a(slot,tile,first,h):
        a=normed(h)
        av[pl.ds(first,BM),:]=a
        atv[slot,:,pl.ds(tile*BM,BM)]=a.T
    def gate_up(i):
        for cp in load_w(i): cp.wait()
        @pl.when(i>=2)
        def _():
            for cp in store_ab(i-2): cp.wait()
        s=lax.rem(i,2)
        w_gate,w_up=(wv[m,s].reshape(D,COLS) for m in range(2))
        for r in range(TILES):
            rows=pl.ds(r*BM,BM)
            g=dot(av[rows,:],w_gate)
            u=dot(av[rows,:],w_up)
            sg=jax.nn.sigmoid(g)
            b=g*sg
            abv[0,s,rows,:]=u*(sg+b*(1-sg))
            abv[1,s,rows,:]=b
            ptv[r,aligned(lax.rem(i,NG),COLS),:]=(b*u).astype(bf).T
        for cp in store_ab(i): cp.start()
    def down(r):
        store_at(0,r).wait()
        for tile in range(DM//BM):
            first=pl.multiple_of(r*DM+tile*BM,BM)
            y=dot(ptv[r*(DM//BM)+tile],wcv[0],0,0).astype(bf)
            h=xv[pl.ds(first,BM),:]+y
            hv[r,pl.ds(tile*BM,BM),:]=h
            put_a(r,tile,first,h)
        store_h(r).start()
        store_at(1,r).start()
    tick(0)
    load_x.wait()
    for r in range(DOWN_STEPS):
        def norm(tile,carry):
            first=pl.multiple_of(r*DM+tile*BM,BM)
            a=normed(xv[pl.ds(first,BM),:])
            av[pl.ds(first,BM),:]=a
            atv[r,:,aligned(tile,BM)]=a.T
            return carry
        lax.fori_loop(0,DM//BM,norm,0)
        store_at(0,r).start()
    def step(t,carry):
        k=t-G_DEPTH-1
        tick(t)
        @pl.when(is_item(k+1))
        def _():
            for cp in load_w(item_of(k+1)): cp.start()
        @pl.when(is_item(k))
        def _(): gate_up(item_of(k))
        @pl.when((k>=NG)&(k<NG+DOWN_STEPS))
        def _(): down(k-NG)
        return carry
    lax.fori_loop(1,F_STEPS+G_DEPTH+1,step,0)
    for r in range(DOWN_STEPS):
        store_at(1,r).wait()
        store_h(r).wait()
    for e in (eg,eu,ed): e.drain()
    for i in (ITEMS-2,ITEMS-1):
        for cp in store_ab(i): cp.wait()
    for l in range(L): store_wc(l).wait()

def forward(x,wg,wu,wd):
    return pl.pallas_call(f_kernel,
        out_shape=[S((ITEMS,*TORUS,R8,COLS),bf)]*2+[S((L*ND,*TORUS,PAD,LANES),bf)]+[S((L,NG,M,COLS),f32)]*2+[
            S((L,TILES,F,BM),bf),S((L,D,M),bf),S((M,D),bf),S((L,F,D),bf)],
        in_specs=[ANY]+[INVMEM]*3,out_specs=[ANY]*9,
        scratch_shapes=[VMEM((L,PAD,D),bf),VMEM((M,D),bf),VMEM((M,D),bf),VMEM((TILES,F,BM),bf),VMEM((L,F,D),bf),VMEM((2,2,*TORUS,R8,COLS),bf),
            VMEM((2,*TORUS,PAD,LANES),bf),VMEM((2,2,M,COLS),f32),VMEM((DOWN_STEPS,D,DM),bf),VMEM((DOWN_STEPS,DM,D),bf),
            DMA,DMA((2,2)),DMA((2,)),DMA((2,2)),DMA((2,)),DMA((DOWN_STEPS,)),DMA((DOWN_STEPS,)),DMA((L,))]+[DMA((n,)) if k==0 else DMA((SLOTS,n)) if k==1 else DMA((SLOTS,)) for stages in (G_STAGES,G_STAGES,D_STAGES) for n in (sum(COPIES[k] for k in stages),) for k in range(3)],
        compiler_params=params(0,62),name="forward")(x,wg,wu,wd)


B_TAIL=NG+1
B_STEPS=B_TAIL+TILES
SEND,DOWN=2,3
S_STAGES=6

class Scatter:
    @staticmethod
    def scratch(rows,n,halves,own=4,ds=2):
        V=lambda *s: VMEM((2,*s),bf)
        A,B=((r.size,c.size) for r,c in halves)
        plane,line=(RING,RING),(RING,)
        return [VMEM((own,*CHIPS,rows,n),f32),VMEM((ds,*CHIPS,rows,n),bf),VMEM((4,*CHIPS,rows,n),bf),
            V(*plane,rows,n),V(*plane,*A),V(*plane,*B),V(2,*plane,rows,n),V(2,*plane,rows,n),VMEM((2,*plane,rows,n),f32),
            V(3,*line,rows,n),V(3,*line,rows,n),VMEM((2,*line,rows,n),f32),V(3,rows,n),V(3,rows,n),DMA((2,Scatter.COPIES)),DMA((2,Scatter.COPIES))]
    COUNT,COPIES=16,11
    def __init__(self,torus,order,out,halves,refs):
        self.t,self.order,self.out,self.halves=torus,order,out,halves
        self.own,self.ds,self.dr,self.a1s,self.a1A,self.a1B,self.a2s,self.a2r,self.t1,self.bs,self.br,self.t2,self.cs,self.cr,*self.sems=refs
    @staticmethod
    def slot(ref,i):
        return lax.rem(i,ref.shape[0])
    def copies(self,stage,i):
        t=self.t
        first,b,a=self.order
        s=lax.rem(i,2)
        k=(0,1,3,5,8)[stage]
        to=(t.pid[a],t.qid[a])
        if stage==0: pieces=[(self.ds.at[self.slot(self.ds,i)],self.dr.at[self.slot(self.dr,i)],t.partner)]
        elif stage==1: pieces=[(self.a1s.at[(s,ALL,ALL,*h)],dst.at[s],to[d]) for d,(h,dst) in enumerate(zip(self.halves,(self.a1A,self.a1B),strict=True))]
        elif stage==2: pieces=[(self.a2s.at[s,d],self.a2r.at[s,d],to[d]) for d in range(2)]
        else:
            src,dst,ids=(self.bs,self.br,t.ringid[b]) if stage==3 else (self.cs,self.cr,t.ringid[first])
            pieces=[(src.at[s,d],dst.at[s,d],ids[d]) for d in range(3)]
        return [remote(src,dst,self.sems,s,k+d,dev) for d,(src,dst,dev) in enumerate(pieces)]
    def run(self,stage,i,column):
        t=self.t
        first,b,a=self.order
        s,o,r=lax.rem(i,2),self.slot(self.own,i),self.slot(self.dr,i)
        if stage>0:
            for cp in self.copies(stage-1,i): cp.wait()
        rem=[k for k in range(3) if k!=a]
        plane=lambda v: self.own[(o,*at(a,v))]+self.dr[(r,*at(a,v))].astype(f32)
        line=lambda v: self.t1[(s,*at(b,v,rem))]
        came=lambda ref: (ref[s,d].astype(f32) for d in range(ref.shape[1]))
        if stage==1:
            self.a1s[s]=plane(t.ring[a][1]).astype(bf)
        elif stage==2:
            for d,to in enumerate((t.p[a],t.q[a])):
                v=plane(to)
                for e,(rows,cols) in enumerate(self.halves):
                    part=v[:,:,rows.start:rows.start+rows.size,cols.start:cols.start+cols.size]
                    if d==e: part=part+(self.a1A,self.a1B)[e][s].astype(f32)
                    self.a2s[s,d,:,:,rows,cols]=part.astype(bf)
        elif stage==3:
            self.t1[s]=sum(came(self.a2r),plane(t.xyz[a]))
            for d,to in enumerate(t.ring[b]): self.bs[s,d]=line(to).astype(bf)
        elif stage==4:
            self.t2[s]=sum(came(self.br),line(t.xyz[b]))
            for d,to in enumerate(t.ring[first]): self.cs[s,d]=self.t2[s,to].astype(bf)
        elif stage==5:
            self.out(column,sum(came(self.cr),self.t2[s,t.xyz[first]]).astype(bf))
        if stage<5:
            for cp in self.copies(stage,i): cp.start()

def split(core,v0,v1):
    return jnp.where(core==0,v0,v1),jnp.where(core==0,v1,v0)

def b_kernel(x,dy,h1,ga,gb,pt,at_,wc,gg,gu,dx,og,ou,od,dgo,duo,
        odp,dhv,atv,both,abv,gsv,wdv,tiles,hv,dhsem,atsem,bothsem,absem,gssem,wdsem,tilesem,hsem,dxsem,*scr):
    torus=Torus()
    layer_of=lambda half: L-1-half
    def prefetch(half,j):
        l,s=layer_of(half),lax.rem(j,2)
        return [pltpu.make_async_copy(o.at[l,j],abv.at[m,s],absem.at[m,s]) for m,o in enumerate((ga,gb))]+[
            pltpu.make_async_copy(wc.at[l,aligned(j,COLS)],wdv.at[s],wdsem.at[s])]
    def load_at(half):
        return pltpu.make_async_copy(at_.at[layer_of(half)],atv,atsem)
    def load_pt(half):
        return [pltpu.make_async_copy(pt.at[aligned(layer_of(half),TILES*F)],both,bothsem.at[0])]
    def load_w(half):
        return [pltpu.make_async_copy(g.at[aligned(layer_of(half),NG*D)],both.at[pl.ds(m*NG*D,NG*D)],bothsem.at[m]) for m,g in enumerate((gg,gu))]
    def store_gs(j):
        s=lax.rem(j,2)
        return [pltpu.make_async_copy(gsv.at[m,s],o.at[j],gssem.at[m,s]) for m,o in enumerate((dgo,duo))]
    def load_tile(r):
        s=lax.rem(r,2)
        return [pltpu.make_async_copy(o.at[:,aligned(r,BM)],tiles.at[m,s],tilesem.at[m,s]) for m,o in enumerate((dgo,duo))]
    def load_h(half,r,go):
        s=lax.rem(r,2)
        for k,h in enumerate((h1,x)):
            @pl.when(half==k)
            def _():
                cp=pltpu.make_async_copy(h.at[aligned(r,BM)],hv.at[s],hsem.at[s])
                cp.start() if go else cp.wait()
    def store_dx(r):
        return pltpu.make_async_copy(dhv.at[aligned(r,BM)],dx.at[aligned(r,BM)],dxsem.at[r])
    def each(copies,go):
        for cp in copies: cp.start() if go else cp.wait()

    load_dh=pltpu.make_async_copy(dy,dhv,dhsem)
    load_dh.start()
    each(prefetch(0,0),True)
    load_at(0).start()
    torus.barrier()
    n=Scatter.COUNT
    def outs(half):
        l=layer_of(half)
        def gate(j,v): og[l,:,aligned(j,COLS)]=v
        def up(j,v): ou[l,:,aligned(j,COLS)]=v
        def down(k,v): odp[l,:,aligned(k,LANES)]=v
        return gate,up,down
    def scatters(half):
        return [Scatter(torus,order,out,h,scr[m*n:(m+1)*n]) for m,(order,out,h) in
            enumerate(zip(ORDERS,outs(half),(HALF_COLS,HALF_COLS,HALF_ROWS),strict=True))]
    eg,eu,ed=scatters(0)

    def tick(half,s):
        eg,eu,ed=scatters(half)
        for stage in reversed(range(S_STAGES)):
            j=s-SEND-stage
            @pl.when((j>=0)&(j<NG))
            def _():
                for e in (eg,eu): e.run(stage,half*NG+j,j)
                @pl.when((j>=DOWN)&(j<DOWN+ND))
                def _(): ed.run(stage,half*ND+j-DOWN,j-DOWN)

    def front(j):
        s=lax.rem(j,2)
        for r in range(TILES):
            rows=pl.ds(r*BM,BM)
            dp=dot(dhv[rows,:],wdv[s],1,1).astype(bf).astype(f32)
            for m in range(2):
                gsv[m,s,rows,:]=(dp*abv[m,s,rows,:]).astype(bf)
    def back(half,j):
        s,i=lax.rem(j,2),half*NG+j
        o,to=Scatter.slot(eg.own,i),Scatter.slot(eg.ds,i)
        for m,e in enumerate((eg,eu)):
            grad=gsv[m,s]
            for k in range(RING):
                v=dot(atv[pl.ds(k*BM,BM),:],grad).reshape(RING*RING,2,R8,COLS)
                own,other=split(torus.c,v[:,0],v[:,1])
                e.own[o,k]=own.reshape(RING,RING,R8,COLS)
                e.ds[to,k]=other.astype(bf).reshape(RING,RING,R8,COLS)
    def grad_down(half,k):
        pair,part=lax.div(k,2),lax.rem(k,2)
        dh=dhv[:,aligned(pair,COLS)]
        item=half*ND+2*pair
        for g in range(EIGHT):
            x,y=part*2+g//RING,g%RING
            first=(x*RING+y)*GROUP
            rows=jnp.concatenate([both[pl.ds(pl.multiple_of(r*F+first,PAD-EIGHT),GROUP),:] for r in range(TILES)],1)
            v=dot(rows,dh)
            for z in range(RING):
                pair=[v[ROWS*d:ROWS*d+ROWS] for d in (2*z,2*z+1)]
                own,other=split(torus.c,*pair)
                other=other.astype(bf)
                for e in range(2):
                    cols=slice(e*LANES,e*LANES+LANES)
                    ed.own[Scatter.slot(ed.own,item+e),x,y,z,0:ROWS,:]=own[:,cols]
                    ed.ds[Scatter.slot(ed.ds,item+e),x,y,z,0:ROWS,:]=other[:,cols]
    def grad_h(half,r):
        s=lax.rem(r,2)
        acc=None
        for j in range(NG):
            for m in range(2):
                v=dot(tiles[m,s,j],both[pl.ds((m*NG+j)*D,D),:],1,1)
                acc=v if acc is None else acc+v
        d=acc.astype(bf).astype(f32)
        h=hv[s].astype(f32)
        scale=rms(h)
        through=jnp.sum(d*h,-1,keepdims=True)*(scale*scale*scale)*(1/D)
        rows=aligned(r,BM)
        dhv[rows,:]=dhv[rows,:]+(d*scale-h*through).astype(bf)
        @pl.when(half==L-1)
        def _(): store_dx(r).start()

    load_dh.wait()
    def step(now,carry):
        half,s=lax.div(now,B_STEPS),lax.rem(now,B_STEPS)
        r=s-B_TAIL
        tick(half,s)
        @pl.when(s<NG-1)
        def _(): each(prefetch(half,s+1),True)
        @pl.when(s==1)
        def _(): each(load_pt(half),True)
        @pl.when(s==B_TAIL-1)
        def _():
            each(store_gs(NG-1),False)
            each(store_gs(NG-2),False)
            each(load_tile(0),True)
            load_h(half,0,True)
            each(load_w(half),True)
        @pl.when(s==B_TAIL)
        def _(): each(load_w(half),False)
        @pl.when((s==B_TAIL)&(half<L-1))
        def _(): load_at(half+1).start()
        @pl.when((s>=B_TAIL)&(s<B_STEPS-1))
        def _():
            each(load_tile(r+1),True)
            load_h(half,r+1,True)
        @pl.when((s==B_STEPS-1)&(half<L-1))
        def _(): each(prefetch(half+1,0),True)
        @pl.when(s<NG)
        def _():
            each(prefetch(half,s),False)
            @pl.when(s>=2)
            def _(): each(store_gs(s-2),False)
        @pl.when(s==1)
        def _(): load_at(half).wait()
        @pl.when(s==DOWN)
        def _(): each(load_pt(half),False)
        @pl.when(s>=B_TAIL)
        def _():
            each(load_tile(r),False)
            load_h(half,r,False)
        @pl.when(s==0)
        def _(): front(s)
        @pl.when((s>0)&(s<DOWN))
        def _():
            front(s); back(half,s-1)
        @pl.when((s>=DOWN)&(s<NG))
        def _():
            front(s); grad_down(half,s-DOWN); back(half,s-1)
        @pl.when(s==NG)
        def _(): back(half,s-1)
        @pl.when(s<NG)
        def _(): each(store_gs(s),True)
        @pl.when(s>=B_TAIL)
        def _(): grad_h(half,r)
        return carry
    lax.fori_loop(0,L*B_STEPS,step,0)
    for r in range(TILES): store_dx(r).wait()
    for l in range(L): od[:,l,:]=odp[l,0:ROWS,:]

def backward(x,dy,h1,ga,gb,pt,at_,wc,gg,gu):
    return pl.pallas_call(b_kernel,
        out_shape=[S((M,D),bf),S((L,R8,F),bf),S((L,R8,F),bf),S((ROWS,L,D),bf)]+[S((NG,M,COLS),bf)]*2,
        in_specs=[ANY]*10,out_specs=[ANY]+[INVMEM]*3+[ANY]*2,
        scratch_shapes=[VMEM((L,PAD,D),bf),VMEM((M,D),bf),VMEM((D,M),bf),VMEM((TILES*F,COLS),bf),VMEM((2,2,M,COLS),f32),VMEM((2,2,M,COLS),bf),
            VMEM((2,COLS,D),bf),VMEM((2,2,NG,BM,COLS),bf),VMEM((2,BM,D),bf),
            DMA,DMA,DMA((2,)),DMA((2,2)),DMA((2,2)),DMA((2,)),DMA((2,2)),DMA((2,)),DMA((TILES,))]
            +Scatter.scratch(R8,COLS,HALF_COLS)*2+Scatter.scratch(PAD,LANES,HALF_ROWS,6,4),
        compiler_params=params(1,63),name="backward")(x,dy,h1,ga,gb,pt,at_,wc,gg,gu)

def finish_kernel(*refs):
    n=len(refs)//4
    src,dst,held,sems=(refs[k*n:k*n+n] for k in range(4))
    def parts(r):
        size=r.shape[0]//4 if r.shape[0]==M else r.shape[0]
        return [pl.ds(k,size) for k in range(0,r.shape[0],size)]
    jobs=[(m,k,p) for m in range(n) for k,p in enumerate(parts(src[m]))]
    load=lambda m,k,p: pltpu.make_async_copy(src[m].at[p],held[m].at[p],sems[m].at[0,k])
    store=lambda m,k,p: pltpu.make_async_copy(held[m].at[p],dst[m].at[p],sems[m].at[1,k])
    for job in jobs: load(*job).start()
    for job in jobs:
        load(*job).wait()
        store(*job).start()
    for job in jobs: store(*job).wait()

def finish(*arrays):
    n=len(arrays)
    return pl.pallas_call(finish_kernel,out_shape=[S(t.shape,t.dtype) for t in arrays],in_specs=[ANY]*n,out_specs=[ANY]*n,
        scratch_shapes=[VMEM(t.shape,t.dtype) for t in arrays]+[DMA((2,4))]*n,
        compiler_params=pltpu.CompilerParams(vmem_limit_bytes=62<<20),name="finish")(*arrays)

def step(x,dy,wg,wu,wd):
    x,dy=x[0],dy[0]
    gg,gu,_,ga,gb,pt,at_,h1,wc=forward(x,wg,wu,jnp.swapaxes(wd,0,1))
    gg,gu=(t.reshape(ITEMS*D,COLS) for t in (gg,gu))
    dx,og,ou,od,_,_=backward(x,dy,h1,ga,gb,pt.reshape(L*TILES*F,COLS),at_,wc,gg,gu)
    dx,og,ou,od=finish(dx,og,ou,od)
    return dx[None],og,ou,jnp.swapaxes(od,0,1)

def solution(mesh):
    tok=P(("rep","dp"),None,None)
    w=P(None,"dp",None)
    o=P("rep","dp",None)
    return jax.shard_map(step,mesh=mesh,in_specs=(tok,tok,w,w,w),out_specs=(tok,o,o,o),check_vma=False)
```
